1024 devices in a mesh: gx: 16 (over y, core), gy: 8 (over x, z_hi), gz: 8 (over z_lo).
Axes of the slice: x: 4, y: 8, z: 16 (z_hi: 2, z_lo: 8; z = z_hi * 8 + z_lo), core: 2. Of those that a mesh axis runs over, the one named last changes fastest.
Arguments:
- density: float32 [128, 128, 1024], P('gx', 'gy', 'gz'), may hold values from 0.7 to 1.6
- momentum: float32 [128, 128, 1024], P('gx', 'gy', 'gz'), may hold values from -7 to 7
- hydrogen: float32 [128, 128, 1024], P('gx', 'gy', 'gz'), may hold values from 0.05 to 1.2
- forced_modes: int32 [96, 3], replicated, may hold values from -3 to 3, as said below
Outputs:
- density_rate: float32 [128, 128, 1024], P('gx', 'gy', 'gz')
- momentum_rate: float32 [128, 128, 1024], P('gx', 'gy', 'gz')
- hydrogen_rate: float32 [128, 128, 1024], P('gx', 'gy', 'gz')
The draws below stay inside these ranges and needn't reach their ends.
Inputs may be any that keep to these rules, and one draw needn't show every extreme that they name: `forced_modes`: each row is a wave vector (kx, ky, kz) with 1 <= kx^2 + ky^2 + kz^2 <= 9; the 96 rows are distinct.
All inputs are finite; a program needn't handle non-finite values.
Results may differ from the reference program's by a relative error of at most 0.0003.
Values sent between devices are 32-bit elements; how exact they have to be, the bound alone decides.
No kernel may reach another device: no remote copies, remote signals or barrier semaphores. Data moves between devices by JAX's collectives and lax.ppermute only.
A program may use at most 32 MiB of HBM per device.

```python
import jax
import jax.numpy as jnp
import numpy as np
from jax import lax

KMAX = 3
MODES = 96
NX = 128
NY = 128
NZ = 1024


def draw_momentum(key, part):
    keys = jax.random.split(key, 6)
    noise = jnp.clip(0.35 * jax.random.normal(keys[0], (NX, NY, NZ), jnp.float32), -1.4, 1.4)
    amp_low = 0.4
    amp_high = 1.0
    total = noise
    for term in range(4):
        sub = jax.random.split(keys[term + 1], 3)
        wavevec = jax.random.randint(sub[0], (3,), 0, 2).astype(jnp.float32)
        phases = jax.random.uniform(sub[1], (3,), jnp.float32, -jnp.pi, jnp.pi)
        amplitude = jax.random.uniform(sub[2], (), jnp.float32, amp_low, amp_high)
        wave_x = jnp.cos(2.0 * jnp.pi * wavevec[0] * jnp.arange(NX, dtype=jnp.float32) / NX + phases[0])
        wave_y = jnp.cos(2.0 * jnp.pi * wavevec[1] * jnp.arange(NY, dtype=jnp.float32) / NY + phases[1])
        wave_z = jnp.cos(2.0 * jnp.pi * wavevec[2] * jnp.arange(NZ, dtype=jnp.float32) / NZ + phases[2])
        total = total + amplitude * wave_x[:, None, None] * wave_y[None, :, None] * wave_z[None, None, :]
    return total.astype(jnp.float32)


def wave_sheet(key, rows, cols, theta_low, theta_high):
    keys = jax.random.split(key, 3)
    theta = jax.random.uniform(keys[0], (3,), jnp.float32, theta_low, theta_high)
    drift = jax.random.uniform(keys[1], (3,), jnp.float32, -0.2, 0.2)
    phase = jax.random.uniform(keys[2], (3,), jnp.float32, -jnp.pi, jnp.pi)
    across = jnp.arange(rows, dtype=jnp.float32)[:, None]
    along = jnp.arange(cols, dtype=jnp.float32)[None, :]
    total = jnp.zeros((rows, cols), jnp.float32)
    for term in range(3):
        total = total + 0.09 * jnp.cos(theta[term] * along + drift[term] * across + phase[term])
    return total


def draw_hydrogen(key, part):
    keys = jax.random.split(key, 3)
    sheet_y = wave_sheet(keys[0], NX, NY, 0.5, 1.05)
    sheet_z = wave_sheet(keys[1], NX, NZ, 0.5, 1.05)
    rough = jnp.clip(0.02 * jax.random.normal(keys[2], (NX, NY, NZ), jnp.float32), -0.045, 0.045)
    smooth = 0.6 + sheet_y[:, :, None] + sheet_z[:, None, :]
    return (smooth * (1.0 + rough)).astype(jnp.float32)


def draw_forced_modes(key, part):
    grid = np.arange(-3, 4)
    triples = np.stack(np.meshgrid(grid, grid, grid, indexing='ij'), -1).reshape(-1, 3)
    radius = np.sum(triples * triples, axis=1)
    valid = triples[(radius >= 1) & (radius <= 9)].astype(np.int32)
    chosen = jax.random.permutation(key, valid.shape[0])[:MODES]
    return jnp.asarray(valid)[chosen].astype(jnp.int32)


def steps_of(rng, shape, pieces, smallest, high):
    gain = 1.0
    for axis_at, shards_of in pieces:
        heights = jax.random.uniform(jax.random.fold_in(jax.random.fold_in(rng, 6), axis_at), (shards_of,), jnp.float32, smallest / len(pieces), high / len(pieces))
        gain = gain * jnp.repeat(jnp.exp(heights), shape[axis_at] // shards_of).reshape((-1,) + (1,) * (len(shape) - 1 - axis_at))
    return gain


def setup_inputs(seed: int = 0) -> dict:
    streams_of = jax.random.split(jax.random.key(seed), 5)
    density = jnp.clip(0.7 + 0.90000004 * jax.random.uniform(streams_of[0], (NX, NY, NZ), jnp.float32) ** steps_of(streams_of[0], (NX, NY, NZ), ((0, 16), (1, 8), (2, 8)), -0.2, 0.2), 0.7, 1.6)
    momentum = draw_momentum(jax.random.fold_in(streams_of[4], 71), 0)
    hydrogen = draw_hydrogen(jax.random.fold_in(streams_of[4], 71), 0)
    forced_modes = draw_forced_modes(jax.random.fold_in(streams_of[4], 71), 0)
    return dict(density=density, momentum=momentum, hydrogen=hydrogen, forced_modes=forced_modes)


FIRST_COEFFS = (0.8, -0.2, 4.0 / 105.0, -1.0 / 280.0)
SECOND_COEFFS = (1.6, -0.2, 8.0 / 315.0, -1.0 / 560.0)
CENTRE_COEFF = -205.0 / 72.0
VISCOSITY = 0.3
DIFFUSIVITY = 1.5
FORCE_POWER = 0.3
ENERGY_EPS = 1e-6
ACTIVATION = 2.0
HIGHEST = lax.Precision.HIGHEST


def first_diff(field, axis):
    total = jnp.zeros_like(field)
    for offset, weight in enumerate(FIRST_COEFFS, 1):
        total = total + weight * (jnp.roll(field, -offset, axis) - jnp.roll(field, offset, axis))
    return total


def second_diff(field, axis):
    total = CENTRE_COEFF * field
    for offset, weight in enumerate(SECOND_COEFFS, 1):
        total = total + weight * (jnp.roll(field, -offset, axis) + jnp.roll(field, offset, axis))
    return total


def wave_tables(start, local, total):
    position = start + jnp.arange(local, dtype=jnp.int32)
    wavenum = jnp.arange(-KMAX, KMAX + 1, dtype=jnp.int32)
    phase = (wavenum[:, None] * position[None, :]) % total
    angle = (2.0 * jnp.pi / total) * phase.astype(jnp.float32)
    return jnp.cos(angle), jnp.sin(angle)


def reference(density, momentum, hydrogen, forced_modes):
    size_x, size_y, size_z = density.shape
    velocity = momentum / density
    cos_x, sin_x = wave_tables(0, size_x, size_x)
    cos_y, sin_y = wave_tables(0, size_y, size_y)
    cos_z, sin_z = wave_tables(0, size_z, size_z)
    flat = velocity.reshape(size_x * size_y, size_z)
    part_re = jnp.dot(cos_z, flat.T, precision=HIGHEST).reshape(-1, size_x, size_y)
    part_im = jnp.dot(sin_z, flat.T, precision=HIGHEST).reshape(-1, size_x, size_y)
    mid_re = jnp.einsum('axy,by->abx', part_re, cos_y, precision=HIGHEST) - jnp.einsum('axy,by->abx', part_im, sin_y, precision=HIGHEST)
    mid_im = jnp.einsum('axy,by->abx', part_re, sin_y, precision=HIGHEST) + jnp.einsum('axy,by->abx', part_im, cos_y, precision=HIGHEST)
    cube_re = jnp.einsum('abx,cx->cba', mid_re, cos_x, precision=HIGHEST) - jnp.einsum('abx,cx->cba', mid_im, sin_x, precision=HIGHEST)
    cube_im = jnp.einsum('abx,cx->cba', mid_re, sin_x, precision=HIGHEST) + jnp.einsum('abx,cx->cba', mid_im, cos_x, precision=HIGHEST)
    width = 2 * KMAX + 1
    code = (forced_modes[:, 0] + KMAX) * width * width + (forced_modes[:, 1] + KMAX) * width + (forced_modes[:, 2] + KMAX)
    selector = (code[:, None] == jnp.arange(width ** 3, dtype=jnp.int32)[None, :]).astype(jnp.float32)
    ncell = float(size_x * size_y * size_z)
    coef_cos = jnp.dot(selector, cube_re.reshape(-1), precision=HIGHEST) / ncell
    coef_sin = jnp.dot(selector, cube_im.reshape(-1), precision=HIGHEST) / ncell
    energy = jnp.sum(coef_cos * coef_cos + coef_sin * coef_sin)
    spec_re = jnp.dot(selector.T, coef_cos, precision=HIGHEST).reshape(width, width, width)
    spec_im = -jnp.dot(selector.T, coef_sin, precision=HIGHEST).reshape(width, width, width)
    step_re = jnp.einsum('abc,ax->xbc', spec_re, cos_x, precision=HIGHEST) - jnp.einsum('abc,ax->xbc', spec_im, sin_x, precision=HIGHEST)
    step_im = jnp.einsum('abc,ax->xbc', spec_re, sin_x, precision=HIGHEST) + jnp.einsum('abc,ax->xbc', spec_im, cos_x, precision=HIGHEST)
    plane_re = jnp.einsum('xbc,by->xyc', step_re, cos_y, precision=HIGHEST) - jnp.einsum('xbc,by->xyc', step_im, sin_y, precision=HIGHEST)
    plane_im = jnp.einsum('xbc,by->xyc', step_re, sin_y, precision=HIGHEST) + jnp.einsum('xbc,by->xyc', step_im, cos_y, precision=HIGHEST)
    low = 2.0 * (jnp.dot(plane_re.reshape(-1, width), cos_z, precision=HIGHEST) - jnp.dot(plane_im.reshape(-1, width), sin_z, precision=HIGHEST))
    force = FORCE_POWER * low.reshape(size_x, size_y, size_z) / (energy + ENERGY_EPS)
    density_rate = -first_diff(momentum, 0)
    lap_mom = second_diff(momentum, 0) + second_diff(momentum, 1) + second_diff(momentum, 2)
    lap_fuel = second_diff(hydrogen, 0) + second_diff(hydrogen, 1) + second_diff(hydrogen, 2)
    momentum_rate = -first_diff(momentum * velocity + density, 0) + VISCOSITY * lap_mom + density * force
    hydrogen_rate = -first_diff(hydrogen * velocity, 0) + DIFFUSIVITY * lap_fuel - hydrogen * jnp.exp(-ACTIVATION * hydrogen / density)
    return density_rate, momentum_rate, hydrogen_rate
```

```python
import functools

import jax
import jax.numpy as jnp
from jax import lax
from jax.experimental import pallas as pl
from jax.experimental.pallas import tpu as pltpu
from jax.sharding import Mesh
from jax.sharding import PartitionSpec as P

GX = ("gx_0", "gx_1")
GY = ("gy_0", "gy_1")
GZ = ("gz",)
FIRST_GROUP = ("gx_0", "gy_0")
SECOND_GROUP = ("gx_1", "gy_1", "gz")

FIRST_COEFFS = (0.8, -0.2, 4.0 / 105.0, -1.0 / 280.0)
SECOND_COEFFS = (1.6, -0.2, 8.0 / 315.0, -1.0 / 560.0)
CENTRE_COEFF = -205.0 / 72.0
VISCOSITY = 0.3
DIFFUSIVITY = 1.5
FORCE_POWER = 0.3
ENERGY_EPS = 1e-06
ACTIVATION = 2.0
HIGHEST = lax.Precision.HIGHEST
LANES = 128
VMEM = pl.BlockSpec(memory_space=pltpu.VMEM)


def row_of(column):
    count = column.shape[0]
    row = lax.broadcasted_iota(jnp.int32, (count, LANES), 0)
    lane = lax.broadcasted_iota(jnp.int32, (count, LANES), 1)
    spread = jnp.broadcast_to(column, (count, LANES))
    return jnp.sum(jnp.where(row == lane, spread, 0.0), axis=0, keepdims=True)


def angles(wave, start, step, count, total):
    index = lax.broadcasted_iota(jnp.int32, (count, LANES), 0)
    position = (start + step * index).astype(jnp.float32)
    phase = wave * position
    phase = phase - total * jnp.round(phase * (1.0 / total))
    return (2.0 * jnp.pi / total) * phase


def partial_kernel(
    full, copies, dens_ref, mom_ref, fuel_ref, modes_ref,
    part_ref, cos_ref, sin_ref, depth_ref,
    xlo_ref, xhi_ref, ylo_ref, yhi_ref, zlo_ref, zhi_ref,
):
    size_x, size_y, size_z = mom_ref.shape
    rows = size_x * size_y
    half = 4
    for n, ref in enumerate((dens_ref, mom_ref, fuel_ref)):
        xlo_ref[n] = ref[0:half]
        xhi_ref[n] = ref[size_x - half : size_x]
    for n, ref in enumerate((mom_ref, fuel_ref)):
        ylo_ref[n] = ref[:, 0:half, :]
        yhi_ref[n] = ref[:, size_y - half : size_y, :]
    turned = [ref[...].reshape(rows, size_z).T for ref in (mom_ref, fuel_ref)]
    zlo_ref[...] = jnp.concatenate([t[0:half] for t in turned], axis=0)
    zhi_ref[...] = jnp.concatenate([t[size_z - half : size_z] for t in turned], axis=0)
    modes = modes_ref[...].astype(jnp.float32)
    wave_x, wave_y, wave_z = (row_of(modes[:, n : n + 1]) for n in range(3))
    base_x = (lax.axis_index("gx_0") * 2 + lax.axis_index("gx_1")) * size_x
    base_y = (lax.axis_index("gy_0") * 2 + lax.axis_index("gy_1")) * size_y
    base_z = lax.axis_index("gz") * size_z
    fine = size_z // 8
    angle = jnp.concatenate(
        [
            angles(wave_x, base_x, 1, size_x, full[0]),
            angles(wave_y, base_y, 1, size_y, full[1]),
            angles(wave_z, base_z, fine, 8, full[2]),
            angles(wave_z, 0, 1, fine, full[2]),
        ],
        axis=0,
    )
    cos, sin = jnp.cos(angle), jnp.sin(angle)
    at_y, at_z, at_f = size_x, size_x + size_y, size_x + size_y + 8
    cy, sy = cos[at_y:at_z], sin[at_y:at_z]
    live = lax.broadcasted_iota(jnp.int32, (1, LANES), 1) < modes_ref.shape[0]
    cf = jnp.where(live, cos[at_f:], 0.0)
    sf = jnp.where(live, sin[at_f:], 0.0)
    for n in range(size_x):
        cx, sx = cos[n : n + 1], sin[n : n + 1]
        cos_ref[n] = cx * cy - sx * sy
        sin_ref[n] = sx * cy + cx * sy
    for n in range(8):
        cz, sz = cos[at_z + n : at_z + n + 1], sin[at_z + n : at_z + n + 1]
        depth_ref[n * fine : (n + 1) * fine, 0:LANES] = cz * cf - sz * sf
        depth_ref[n * fine : (n + 1) * fine, LANES:] = sz * cf + cz * sf
    velocity = (mom_ref[...] / dens_ref[...]).reshape(rows, size_z)
    along = jnp.dot(velocity, depth_ref[...], precision=HIGHEST, preferred_element_type=jnp.float32)
    real, imag = along[:, 0:LANES], along[:, LANES:]
    cos_xy = cos_ref[...].reshape(rows, LANES)
    sin_xy = sin_ref[...].reshape(rows, LANES)
    part_cos = jnp.sum(cos_xy * real - sin_xy * imag, axis=0, keepdims=True)
    part_sin = jnp.sum(sin_xy * real + cos_xy * imag, axis=0, keepdims=True)
    both = jnp.concatenate([part_cos, part_sin], axis=0)
    part_ref[...] = jnp.broadcast_to(both[None], (copies, 2, LANES))


def partial_sums(density, momentum, hydrogen, modes, full, copies):
    size_x, size_y, size_z = density.shape
    f32 = jnp.float32
    shapes = (
        (copies, 2, LANES),
        (size_x, size_y, LANES),
        (size_x, size_y, LANES),
        (size_z, 2 * LANES),
        (3, 4, size_y, size_z),
        (3, 4, size_y, size_z),
        (2, size_x, 4, size_z),
        (2, size_x, 4, size_z),
        (8, size_x * size_y),
        (8, size_x * size_y),
    )
    return pl.pallas_call(
        functools.partial(partial_kernel, full, copies),
        out_shape=[jax.ShapeDtypeStruct(s, f32) for s in shapes],
        in_specs=[VMEM] * 4,
        out_specs=[VMEM] * len(shapes),
        compiler_params=pltpu.CompilerParams(vmem_limit_bytes=16 << 20),
        name="partial_sums",
    )(density, momentum, hydrogen, modes)


def first_diff(planes, at):
    total = None
    for offset, weight in enumerate(FIRST_COEFFS, 1):
        term = weight * (planes[at + offset] - planes[at - offset])
        total = term if total is None else total + term
    return total


def second_diff(pick):
    total = CENTRE_COEFF * pick(0)
    for offset, weight in enumerate(SECOND_COEFFS, 1):
        total = total + weight * (pick(offset) + pick(-offset))
    return total


def final_kernel(
    ncell, dens_ref, mom_ref, fuel_ref, summed_ref, cos_ref, sin_ref, depth_ref,
    xbefore_ref, xafter_ref, ybefore_ref, yafter_ref, zbefore_ref, zafter_ref,
    dens_out, mom_out, fuel_out, force_ref,
):
    size_x, size_y, size_z = mom_ref.shape
    rows = size_x * size_y
    total = jnp.sum(summed_ref[...], axis=0) * (1.0 / ncell)
    energy = jnp.sum(total * total)
    scaled = total * (2.0 * FORCE_POWER / (energy + ENERGY_EPS))
    coef_cos, coef_sin = scaled[0:1], scaled[1:2]
    cos_xy = cos_ref[...].reshape(rows, LANES)
    sin_xy = sin_ref[...].reshape(rows, LANES)
    side = jnp.concatenate(
        [coef_cos * cos_xy + coef_sin * sin_xy, coef_sin * cos_xy - coef_cos * sin_xy], axis=1
    )
    force_ref[...] = lax.dot_general(
        side, depth_ref[...], (((1,), (1,)), ((), ())), precision=HIGHEST,
        preferred_element_type=jnp.float32,
    ).reshape(size_x, size_y, size_z)
    gap = jnp.zeros((56, rows), jnp.float32)
    before, after = zbefore_ref[...], zafter_ref[...]
    turned = jnp.concatenate(
        [after[0:4], gap, before[4:8], after[4:8], gap, before[0:4]], axis=0
    ).T
    halo = [turned, pltpu.roll(turned, 64, 1)]
    lane = lax.broadcasted_iota(jnp.int32, (1, size_z), 1)
    dens, mom, fuel = (
        [xbefore_ref[n, i] for i in range(4)] + [ref[i] for i in range(size_x)] + [xafter_ref[n, i] for i in range(4)]
        for n, ref in enumerate((dens_ref, mom_ref, fuel_ref))
    )
    vel = [m / d for m, d in zip(mom, dens)]
    mom_flux = [m * v + d for m, v, d in zip(mom, vel, dens)]
    fuel_flux = [f * v for f, v in zip(fuel, vel)]
    for i in range(size_x):
        at = i + 4
        dens_out[i] = -first_diff(mom, at)
        spread = []
        for n, planes in enumerate((mom, fuel)):
            here = planes[at]
            tall = jnp.concatenate([ybefore_ref[n, i], here, yafter_ref[n, i]], axis=0)
            edge = halo[n][i * size_y : (i + 1) * size_y]

            def along_z(offset):
                if offset == 0:
                    return here
                if offset > 0:
                    return pltpu.roll(jnp.where(lane < offset, edge, here), size_z - offset, 1)
                return pltpu.roll(jnp.where(lane >= size_z + offset, edge, here), -offset, 1)

            spread.append(
                second_diff(lambda o: planes[at + o])
                + second_diff(lambda o: tall[4 + o : 4 + o + size_y])
                + second_diff(along_z)
            )
        mom_out[i] = -first_diff(mom_flux, at) + VISCOSITY * spread[0] + dens[at] * force_ref[i]
        fuel_out[i] = (
            -first_diff(fuel_flux, at) + DIFFUSIVITY * spread[1]
            - fuel[at] * jnp.exp(-ACTIVATION * fuel[at] / dens[at])
        )


def final_rates(density, momentum, hydrogen, summed, cos, sin, depth, halos, ncell):
    shape = density.shape
    return pl.pallas_call(
        functools.partial(final_kernel, ncell),
        out_shape=[jax.ShapeDtypeStruct(shape, jnp.float32)] * 3,
        in_specs=[VMEM] * 13,
        out_specs=[VMEM] * 3,
        scratch_shapes=[pltpu.VMEM(shape, jnp.float32)],
        compiler_params=pltpu.CompilerParams(vmem_limit_bytes=16 << 20),
        name="final_rates",
    )(density, momentum, hydrogen, summed, cos, sin, depth, *halos)


def shift_up(x, axes):
    size = lax.axis_size(axes)
    return lax.ppermute(x, axes, [(i, (i + 1) % size) for i in range(size)])


def shift_down(x, axes):
    size = lax.axis_size(axes)
    return lax.ppermute(x, axes, [((i + 1) % size, i) for i in range(size)])


def exchange(x, axes):
    return lax.all_to_all(x, axes, 0, 0, tiled=True)


def per_device(density, momentum, hydrogen, forced_modes):
    size_x, size_y, size_z = density.shape
    full = (
        size_x * lax.axis_size(GX),
        size_y * lax.axis_size(GY),
        size_z * lax.axis_size(GZ),
    )
    first, second = lax.axis_size(FIRST_GROUP), lax.axis_size(SECOND_GROUP)
    part, cos, sin, depth, xlo, xhi, ylo, yhi, zlo, zhi = partial_sums(
        density, momentum, hydrogen, forced_modes, full, first
    )
    halos = (
        shift_up(xhi, GX), shift_down(xlo, GX),
        shift_up(yhi, GY), shift_down(ylo, GY),
        shift_up(zhi, GZ), shift_down(zlo, GZ),
    )
    plane = jnp.sum(exchange(part, FIRST_GROUP), axis=0)
    summed = exchange(jnp.broadcast_to(plane[None], (second,) + plane.shape), SECOND_GROUP)
    return tuple(
        final_rates(
            density, momentum, hydrogen, summed, cos, sin, depth, halos,
            float(full[0] * full[1] * full[2]),
        )
    )


def solution(mesh):
    split = Mesh(
        mesh.devices.reshape(8, 2, 4, 2, mesh.shape["gz"]), ("gx_0", "gx_1", "gy_0", "gy_1", "gz")
    )
    field = P(GX, GY, "gz")
    return jax.shard_map(
        per_device, mesh=split, in_specs=(field, field, field, P()),
        out_specs=(field, field, field), check_vma=False,
    )
```

```python
import functools

import jax
import jax.numpy as jnp
from jax import lax
from jax.experimental import pallas as pl
from jax.experimental.pallas import tpu as pltpu
from jax.sharding import Mesh
from jax.sharding import PartitionSpec as P


GX = ("gx_0", "gx_1")
GY = ("gy_0", "gy_1")
GZ = ("gz",)
FIRST_GROUP = ("gx_0", "gy_0")
SECOND_GROUP = ("gx_1", "gy_1", "gz")

FIRST_COEFFS = (0.8, -0.2, 4.0 / 105.0, -1.0 / 280.0)
SECOND_COEFFS = (1.6, -0.2, 8.0 / 315.0, -1.0 / 560.0)
CENTRE_COEFF = -205.0 / 72.0
VISCOSITY = 0.3
DIFFUSIVITY = 1.5
FORCE_POWER = 0.3
ENERGY_EPS = 1e-06
ACTIVATION = 2.0
HIGHEST = lax.Precision.HIGHEST
LANES = 128
VMEM = pl.BlockSpec(memory_space=pltpu.VMEM)


def odd(axis):
    return lax.rem(lax.axis_index(axis), 2) == 1


def angles(wave, start, step, count, total):
    index = lax.broadcasted_iota(jnp.int32, (count, LANES), 0)
    position = (start + step * index).astype(jnp.float32)
    phase = wave * position
    phase = phase - total * jnp.round(phase * (1.0 / total))
    return (2.0 * jnp.pi / total) * phase


def partial_kernel(
    full, copies, dens_hbm, mom_hbm, fuel_hbm, modes_ref,
    part_ref, cos_ref, sin_ref, depth_ref,
    xa_ref, xb_ref, ya_ref, yb_ref, za_ref, zb_ref,
    dens_ref, mom_ref, fuel_ref, sems,
):
    size_x, size_y, size_z = mom_ref.shape
    rows = size_x * size_y
    half = 4
    loads = [
        pltpu.make_async_copy(src, dst, sems.at[n])
        for n, (src, dst) in enumerate(((mom_hbm, mom_ref), (dens_hbm, dens_ref), (fuel_hbm, fuel_ref)))
    ]
    for load in loads:
        load.start()
    modes = modes_ref[...].astype(jnp.float32)
    spare = jnp.zeros((1, LANES - modes.shape[1]), jnp.float32)
    wave_x, wave_y, wave_z = (jnp.concatenate([modes[n : n + 1], spare], axis=1) for n in range(3))
    base_x = (lax.axis_index("gx_0") * 2 + lax.axis_index("gx_1")) * size_x
    base_y = (lax.axis_index("gy_0") * 2 + lax.axis_index("gy_1")) * size_y
    base_z = lax.axis_index("gz") * size_z
    fine = size_z // 8
    angle = jnp.concatenate(
        [
            angles(wave_x, base_x, 1, size_x, full[0]),
            angles(wave_y, base_y, 1, size_y, full[1]),
            angles(wave_z, base_z, fine, 8, full[2]),
            angles(wave_z, 0, 1, fine, full[2]),
        ],
        axis=0,
    )
    cos, sin = jnp.cos(angle), jnp.sin(angle)
    at_y, at_z, at_f = size_x, size_x + size_y, size_x + size_y + 8
    cy, sy = cos[at_y:at_z], sin[at_y:at_z]
    live = lax.broadcasted_iota(jnp.int32, (1, LANES), 1) < modes.shape[1]
    cf = jnp.where(live, cos[at_f:], 0.0)
    sf = jnp.where(live, sin[at_f:], 0.0)
    for n in range(size_x):
        cx, sx = cos[n : n + 1], sin[n : n + 1]
        cos_ref[n] = cx * cy - sx * sy
        sin_ref[n] = sx * cy + cx * sy
    for n in range(8):
        cz, sz = cos[at_z + n : at_z + n + 1], sin[at_z + n : at_z + n + 1]
        depth_ref[n * fine : (n + 1) * fine, 0:LANES] = cz * cf - sz * sf
        depth_ref[n * fine : (n + 1) * fine, LANES:] = sz * cf + cz * sf
    loads[0].wait()
    loads[1].wait()
    velocity = (mom_ref[...] / dens_ref[...]).reshape(rows, size_z)
    along = jnp.dot(velocity, depth_ref[...], precision=HIGHEST, preferred_element_type=jnp.float32)
    real, imag = along[:, 0:LANES], along[:, LANES:]
    cos_xy = cos_ref[...].reshape(rows, LANES)
    sin_xy = sin_ref[...].reshape(rows, LANES)
    part_cos = jnp.sum(cos_xy * real - sin_xy * imag, axis=0, keepdims=True)
    part_sin = jnp.sum(sin_xy * real + cos_xy * imag, axis=0, keepdims=True)
    both = jnp.concatenate([part_cos, part_sin], axis=0)
    part_ref[...] = jnp.broadcast_to(both[None], (copies, 2, LANES))
    loads[2].wait()
    odd_x, odd_y, odd_z = odd("gx_1"), odd("gy_1"), odd("gz")
    for n, ref in enumerate((dens_ref, mom_ref, fuel_ref)):
        low, high = ref[0:half], ref[size_x - half : size_x]
        xa_ref[n] = jnp.where(odd_x, low, high)
        xb_ref[n] = jnp.where(odd_x, high, low)
    for n, ref in enumerate((mom_ref, fuel_ref)):
        low, high = ref[:, 0:half, :], ref[:, size_y - half : size_y, :]
        ya_ref[n] = jnp.where(odd_y, low, high)
        yb_ref[n] = jnp.where(odd_y, high, low)
    turned = [ref[...].reshape(rows, size_z).T for ref in (mom_ref, fuel_ref)]
    low = jnp.concatenate([t[0:half] for t in turned], axis=0)
    high = jnp.concatenate([t[size_z - half : size_z] for t in turned], axis=0)
    za_ref[...] = jnp.where(odd_z, low, high)
    zb_ref[...] = jnp.where(odd_z, high, low)


def partial_sums(density, momentum, hydrogen, modes, full, copies):
    size_x, size_y, size_z = density.shape
    f32 = jnp.float32
    shapes = (
        (copies, 2, LANES),
        (size_x, size_y, LANES),
        (size_x, size_y, LANES),
        (size_z, 2 * LANES),
        (3, 4, size_y, size_z),
        (3, 4, size_y, size_z),
        (2, size_x, 4, size_z),
        (2, size_x, 4, size_z),
        (8, size_x * size_y),
        (8, size_x * size_y),
    )
    return pl.pallas_call(
        functools.partial(partial_kernel, full, copies),
        out_shape=[jax.ShapeDtypeStruct(s, f32) for s in shapes],
        in_specs=[pl.BlockSpec(memory_space=pltpu.HBM)] * 3 + [VMEM],
        out_specs=[VMEM] * len(shapes),
        scratch_shapes=[pltpu.VMEM(density.shape, f32)] * 3 + [pltpu.SemaphoreType.DMA((3,))],
        compiler_params=pltpu.CompilerParams(vmem_limit_bytes=16 << 20),
        name="partial_sums",
    )(density, momentum, hydrogen, modes)


def spread_kernel(parts_ref, out_ref):
    out_ref[...] = jnp.broadcast_to(jnp.sum(parts_ref[...], axis=0, keepdims=True), out_ref.shape)


def summed_copies(parts, copies):
    return pl.pallas_call(
        spread_kernel,
        out_shape=jax.ShapeDtypeStruct((copies,) + parts.shape[1:], jnp.float32),
        in_specs=[VMEM],
        out_specs=VMEM,
        compiler_params=pltpu.CompilerParams(vmem_limit_bytes=4 << 20),
        name="summed_copies",
    )(parts)


def first_diff(planes, at):
    total = None
    for offset, weight in enumerate(FIRST_COEFFS, 1):
        term = weight * (planes[at + offset] - planes[at - offset])
        total = term if total is None else total + term
    return total


def second_diff(pick):
    total = CENTRE_COEFF * pick(0)
    for offset, weight in enumerate(SECOND_COEFFS, 1):
        total = total + weight * (pick(offset) + pick(-offset))
    return total


def final_kernel(
    ncell, dens_ref, mom_ref, fuel_ref, summed_ref, cos_ref, sin_ref, depth_ref,
    xa_ref, xb_ref, ya_ref, yb_ref, za_ref, zb_ref,
    dens_out, mom_out, fuel_out, force_ref,
):
    size_x, size_y, size_z = mom_ref.shape
    rows = size_x * size_y
    total = jnp.sum(summed_ref[...], axis=0) * (1.0 / ncell)
    energy = jnp.sum(total * total)
    scaled = total * (2.0 * FORCE_POWER / (energy + ENERGY_EPS))
    coef_cos, coef_sin = scaled[0:1], scaled[1:2]
    cos_xy = cos_ref[...].reshape(rows, LANES)
    sin_xy = sin_ref[...].reshape(rows, LANES)
    side = jnp.concatenate(
        [coef_cos * cos_xy + coef_sin * sin_xy, coef_sin * cos_xy - coef_cos * sin_xy], axis=1
    )
    force_ref[...] = lax.dot_general(
        side, depth_ref[...], (((1,), (1,)), ((), ())), precision=HIGHEST,
        preferred_element_type=jnp.float32,
    ).reshape(size_x, size_y, size_z)
    gap = jnp.zeros((56, rows), jnp.float32)
    odd_x, odd_y, odd_z = odd("gx_1"), odd("gy_1"), odd("gz")
    before = jnp.where(odd_z, za_ref[...], zb_ref[...])
    after = jnp.where(odd_z, zb_ref[...], za_ref[...])
    turned = jnp.concatenate(
        [after[0:4], gap, before[4:8], after[4:8], gap, before[0:4]], axis=0
    ).T
    halo = [turned, pltpu.roll(turned, 64, 1)]
    lane = lax.broadcasted_iota(jnp.int32, (1, size_z), 1)
    dens, mom, fuel = (
        [jnp.where(odd_x, xa_ref[n, i], xb_ref[n, i]) for i in range(4)]
        + [ref[i] for i in range(size_x)]
        + [jnp.where(odd_x, xb_ref[n, i], xa_ref[n, i]) for i in range(4)]
        for n, ref in enumerate((dens_ref, mom_ref, fuel_ref))
    )
    vel = [m / d for m, d in zip(mom, dens)]
    mom_flux = [m * v + d for m, v, d in zip(mom, vel, dens)]
    fuel_flux = [f * v for f, v in zip(fuel, vel)]
    for i in range(size_x):
        at = i + 4
        dens_out[i] = -first_diff(mom, at)
        spread = []
        for n, planes in enumerate((mom, fuel)):
            here = planes[at]
            ya, yb = ya_ref[n, i], yb_ref[n, i]
            tall = jnp.concatenate([jnp.where(odd_y, ya, yb), here, jnp.where(odd_y, yb, ya)], axis=0)
            edge = halo[n][i * size_y : (i + 1) * size_y]

            def along_z(offset):
                if offset == 0:
                    return here
                if offset > 0:
                    return pltpu.roll(jnp.where(lane < offset, edge, here), size_z - offset, 1)
                return pltpu.roll(jnp.where(lane >= size_z + offset, edge, here), -offset, 1)

            spread.append(
                second_diff(lambda o: planes[at + o])
                + second_diff(lambda o: tall[4 + o : 4 + o + size_y])
                + second_diff(along_z)
            )
        mom_out[i] = -first_diff(mom_flux, at) + VISCOSITY * spread[0] + dens[at] * force_ref[i]
        fuel_out[i] = (
            -first_diff(fuel_flux, at) + DIFFUSIVITY * spread[1]
            - fuel[at] * jnp.exp(-ACTIVATION * fuel[at] / dens[at])
        )


def final_rates(density, momentum, hydrogen, summed, cos, sin, depth, halos, ncell):
    shape = density.shape
    return pl.pallas_call(
        functools.partial(final_kernel, ncell),
        out_shape=[jax.ShapeDtypeStruct(shape, jnp.float32)] * 3,
        in_specs=[VMEM] * 13,
        out_specs=[VMEM] * 3,
        scratch_shapes=[pltpu.VMEM(shape, jnp.float32)],
        compiler_params=pltpu.CompilerParams(vmem_limit_bytes=16 << 20),
        name="final_rates",
    )(density, momentum, hydrogen, summed, cos, sin, depth, *halos)


def swap(x, axes, shift):
    size = lax.axis_size(axes)
    pairs = [((i + shift) % size, (i + 1 + shift) % size) for i in range(0, size, 2)]
    return lax.ppermute(x, axes, pairs + [(j, i) for i, j in pairs])


def exchange(x, axes):
    return lax.all_to_all(x, axes, 0, 0, tiled=True)


def per_device(density, momentum, hydrogen, forced_modes):
    size_x, size_y, size_z = density.shape
    full = (
        size_x * lax.axis_size(GX),
        size_y * lax.axis_size(GY),
        size_z * lax.axis_size(GZ),
    )
    first, second = lax.axis_size(FIRST_GROUP), lax.axis_size(SECOND_GROUP)
    part, cos, sin, depth, xa, xb, ya, yb, za, zb = partial_sums(
        density, momentum, hydrogen, forced_modes.T, full, first
    )
    part = exchange(part, FIRST_GROUP)
    ya, yb = swap(ya, GY, 0), swap(yb, GY, 1)
    part = summed_copies(part, second)
    part = exchange(part, SECOND_GROUP)
    xa, xb = swap(xa, GX, 0), swap(xb, GX, 1)
    za, zb = swap(za, GZ, 0), swap(zb, GZ, 1)
    rates = final_rates(
        density, momentum, hydrogen, part, cos, sin, depth, (xa, xb, ya, yb, za, zb),
        float(full[0] * full[1] * full[2]),
    )
    return tuple(rates)


def solution(mesh):
    split = Mesh(
        mesh.devices.reshape(8, 2, 4, 2, mesh.shape["gz"]), ("gx_0", "gx_1", "gy_0", "gy_1", "gz")
    )
    field = P(GX, GY, "gz")
    return jax.shard_map(
        per_device, mesh=split, in_specs=(field, field, field, P()),
        out_specs=(field, field, field), check_vma=False,
    )
```

```python
import functools

import jax
import jax.numpy as jnp
from jax import lax
from jax.experimental import pallas as pl
from jax.experimental.pallas import tpu as pltpu
from jax.sharding import Mesh
from jax.sharding import PartitionSpec as P


GX = ("gx_0", "gx_1")
GY = ("gy_0", "gy_1")
GZ = ("gz",)
FIRST_GROUP = ("gx_0", "gy_0")
RING = ("gy_1", "gz")
SECOND_GROUP = ("gx_1", "gy_1", "gz")

FIRST_COEFFS = (0.8, -0.2, 4.0 / 105.0, -1.0 / 280.0)
SECOND_COEFFS = (1.6, -0.2, 8.0 / 315.0, -1.0 / 560.0)
CENTRE_COEFF = -205.0 / 72.0
VISCOSITY = 0.3
DIFFUSIVITY = 1.5
FORCE_POWER = 0.3
ENERGY_EPS = 1e-06
ACTIVATION = 2.0
HIGHEST = lax.Precision.HIGHEST
LANES = 128
VMEM = pl.BlockSpec(memory_space=pltpu.VMEM)


def odd(axis):
    return lax.rem(lax.axis_index(axis), 2) == 1


def angles(wave, start, step, count, total):
    index = lax.broadcasted_iota(jnp.int32, (count, LANES), 0)
    position = (start + step * index).astype(jnp.float32)
    phase = wave * position
    phase = phase - total * jnp.round(phase * (1.0 / total))
    return (2.0 * jnp.pi / total) * phase


def partial_kernel(
    full, copies, dens_hbm, mom_hbm, fuel_hbm, modes_hbm,
    part_ref, cos_ref, sin_ref, depth_ref,
    xa_ref, xb_ref, sides_ref, za_ref, zb_ref,
    dens_ref, mom_ref, fuel_ref, modes_ref, sems,
):
    size_x, size_y, size_z = mom_ref.shape
    rows = size_x * size_y
    half = 4
    loads = [
        pltpu.make_async_copy(src, dst, sems.at[n])
        for n, (src, dst) in enumerate(
            ((modes_hbm, modes_ref), (mom_hbm, mom_ref), (dens_hbm, dens_ref), (fuel_hbm, fuel_ref))
        )
    ]
    for load in loads:
        load.start()
    loads[0].wait()
    modes = modes_ref[...].astype(jnp.float32)
    spare = jnp.zeros((1, LANES - modes.shape[1]), jnp.float32)
    wave_x, wave_y, wave_z = (jnp.concatenate([modes[n : n + 1], spare], axis=1) for n in range(3))
    base_x = (lax.axis_index("gx_0") * 2 + lax.axis_index("gx_1")) * size_x
    base_y = (lax.axis_index("gy_0") * 2 + lax.axis_index("gy_1")) * size_y
    base_z = lax.axis_index("gz") * size_z
    fine = size_z // 8
    angle = jnp.concatenate(
        [
            angles(wave_x, base_x, 1, size_x, full[0]),
            angles(wave_y, base_y, 1, size_y, full[1]),
            angles(wave_z, base_z, fine, 8, full[2]),
            angles(wave_z, 0, 1, fine, full[2]),
        ],
        axis=0,
    )
    cos, sin = jnp.cos(angle), jnp.sin(angle)
    at_y, at_z, at_f = size_x, size_x + size_y, size_x + size_y + 8
    cy, sy = cos[at_y:at_z], sin[at_y:at_z]
    live = lax.broadcasted_iota(jnp.int32, (1, LANES), 1) < modes.shape[1]
    cf = jnp.where(live, cos[at_f:], 0.0)
    sf = jnp.where(live, sin[at_f:], 0.0)
    for n in range(size_x):
        cx, sx = cos[n : n + 1], sin[n : n + 1]
        cos_ref[n] = cx * cy - sx * sy
        sin_ref[n] = sx * cy + cx * sy
    for n in range(8):
        cz, sz = cos[at_z + n : at_z + n + 1], sin[at_z + n : at_z + n + 1]
        depth_ref[n * fine : (n + 1) * fine, 0:LANES] = cz * cf - sz * sf
        depth_ref[n * fine : (n + 1) * fine, LANES:] = sz * cf + cz * sf
    loads[1].wait()
    loads[2].wait()
    velocity = (mom_ref[...] / dens_ref[...]).reshape(rows, size_z)
    along = jnp.dot(velocity, depth_ref[...], precision=HIGHEST, preferred_element_type=jnp.float32)
    real, imag = along[:, 0:LANES], along[:, LANES:]
    cos_xy = cos_ref[...].reshape(rows, LANES)
    sin_xy = sin_ref[...].reshape(rows, LANES)
    part_cos = jnp.sum(cos_xy * real - sin_xy * imag, axis=0, keepdims=True)
    part_sin = jnp.sum(sin_xy * real + cos_xy * imag, axis=0, keepdims=True)
    both = jnp.concatenate([part_cos, part_sin], axis=0)
    part_ref[...] = jnp.broadcast_to(both[None], (copies, 2, LANES))
    loads[3].wait()
    odd_x, odd_y, odd_z = odd("gx_1"), odd("gy_1"), odd("gz")
    for n, ref in enumerate((dens_ref, mom_ref, fuel_ref)):
        low, high = ref[0:half], ref[size_x - half : size_x]
        xa_ref[n] = jnp.where(odd_x, low, high)
        xb_ref[n] = jnp.where(odd_x, high, low)
    for n, ref in enumerate((mom_ref, fuel_ref)):
        low, high = ref[:, 0:half, :], ref[:, size_y - half : size_y, :]
        sides_ref[n * size_x : (n + 1) * size_x] = jnp.where(odd_y, low, high)
        sides_ref[(n + 2) * size_x : (n + 3) * size_x] = jnp.where(odd_y, high, low)
    turned = [ref[...].reshape(rows, size_z).T for ref in (mom_ref, fuel_ref)]
    low = jnp.concatenate([t[0:half] for t in turned], axis=0)
    high = jnp.concatenate([t[size_z - half : size_z] for t in turned], axis=0)
    za_ref[...] = jnp.where(odd_z, low, high)
    zb_ref[...] = jnp.where(odd_z, high, low)


def partial_sums(density, momentum, hydrogen, modes, full, copies):
    size_x, size_y, size_z = density.shape
    f32 = jnp.float32
    shapes = (
        (copies, 2, LANES),
        (size_x, size_y, LANES),
        (size_x, size_y, LANES),
        (size_z, 2 * LANES),
        (3, 4, size_y, size_z),
        (3, 4, size_y, size_z),
        (4 * size_x, 4, size_z),
        (8, size_x * size_y),
        (8, size_x * size_y),
    )
    density, momentum, hydrogen, modes = (
        pltpu.with_memory_space_constraint(f, pltpu.HBM) for f in (density, momentum, hydrogen, modes)
    )
    return pl.pallas_call(
        functools.partial(partial_kernel, full, copies),
        out_shape=[jax.ShapeDtypeStruct(s, f32) for s in shapes],
        in_specs=[pl.BlockSpec(memory_space=pltpu.HBM)] * 4,
        out_specs=[VMEM] * len(shapes),
        scratch_shapes=[pltpu.VMEM(density.shape, f32)] * 3
        + [pltpu.VMEM(modes.shape, modes.dtype), pltpu.SemaphoreType.DMA((4,))],
        compiler_params=pltpu.CompilerParams(vmem_limit_bytes=16 << 20),
        name="partial_sums",
    )(density, momentum, hydrogen, modes)


def spread_kernel(parts_ref, out_ref):
    out_ref[...] = jnp.broadcast_to(jnp.sum(parts_ref[...], axis=0, keepdims=True), out_ref.shape)


def summed_copies(parts, copies):
    return pl.pallas_call(
        spread_kernel,
        out_shape=jax.ShapeDtypeStruct((copies,) + parts.shape[1:], jnp.float32),
        in_specs=[VMEM],
        out_specs=VMEM,
        compiler_params=pltpu.CompilerParams(vmem_limit_bytes=4 << 20),
        name="summed_copies",
    )(parts)


def pack_kernel(sides_ref, depth_ref, out_ref):
    count = sides_ref.shape[0]
    out_ref[0:count] = sides_ref[...]
    out_ref[count] = depth_ref[0:4]
    out_ref[count + 1] = depth_ref[4:8]


def packed(sides, depth):
    return pl.pallas_call(
        pack_kernel,
        out_shape=jax.ShapeDtypeStruct((sides.shape[0] + 2,) + sides.shape[1:], jnp.float32),
        in_specs=[VMEM] * 2,
        out_specs=VMEM,
        compiler_params=pltpu.CompilerParams(vmem_limit_bytes=4 << 20),
        name="packed",
    )(sides, depth)


def first_diff(planes, at):
    total = None
    for offset, weight in enumerate(FIRST_COEFFS, 1):
        term = weight * (planes[at + offset] - planes[at - offset])
        total = term if total is None else total + term
    return total


def second_diff(pick):
    total = CENTRE_COEFF * pick(0)
    for offset, weight in enumerate(SECOND_COEFFS, 1):
        total = total + weight * (pick(offset) + pick(-offset))
    return total


def final_kernel(
    ncell, dens_ref, mom_ref, fuel_ref, summed_ref, cos_ref, sin_ref, depth_ref,
    xa_ref, xb_ref, traded_ref, relayed_ref, za_ref, zb_ref,
    dens_out, mom_out, fuel_out, force_ref,
):
    size_x, size_y, size_z = mom_ref.shape
    rows = size_x * size_y
    total = jnp.sum(summed_ref[...], axis=0) * (1.0 / ncell)
    energy = jnp.sum(total * total)
    scaled = total * (2.0 * FORCE_POWER / (energy + ENERGY_EPS))
    coef_cos, coef_sin = scaled[0:1], scaled[1:2]
    cos_xy = cos_ref[...].reshape(rows, LANES)
    sin_xy = sin_ref[...].reshape(rows, LANES)
    side = jnp.concatenate(
        [coef_cos * cos_xy + coef_sin * sin_xy, coef_sin * cos_xy - coef_cos * sin_xy], axis=1
    )
    force_ref[...] = lax.dot_general(
        side, depth_ref[...], (((1,), (1,)), ((), ())), precision=HIGHEST,
        preferred_element_type=jnp.float32,
    ).reshape(size_x, size_y, size_z)
    gap = jnp.zeros((56, rows), jnp.float32)
    odd_x, odd_y, odd_z = odd("gx_1"), odd("gy_1"), odd("gz")
    place = lax.axis_index("gz")
    at_end = jnp.logical_or(place == 0, place == lax.axis_size("gz") - 1)
    za, zb = za_ref[...], zb_ref[...]
    swapped = jnp.concatenate([traded_ref[4 * size_x], traded_ref[4 * size_x + 1]], axis=0)
    zb = jnp.where(at_end, swapped, zb)
    before = jnp.where(odd_z, za, zb)
    after = jnp.where(odd_z, zb, za)
    turned = jnp.concatenate(
        [after[0:4], gap, before[4:8], after[4:8], gap, before[0:4]], axis=0
    ).T
    halo = [turned, pltpu.roll(turned, 64, 1)]
    lane = lax.broadcasted_iota(jnp.int32, (1, size_z), 1)
    dens, mom, fuel = (
        [jnp.where(odd_x, xa_ref[n, i], xb_ref[n, i]) for i in range(4)]
        + [ref[i] for i in range(size_x)]
        + [jnp.where(odd_x, xb_ref[n, i], xa_ref[n, i]) for i in range(4)]
        for n, ref in enumerate((dens_ref, mom_ref, fuel_ref))
    )
    vel = [m / d for m, d in zip(mom, dens)]
    mom_flux = [m * v + d for m, v, d in zip(mom, vel, dens)]
    fuel_flux = [f * v for f, v in zip(fuel, vel)]
    for i in range(size_x):
        at = i + 4
        dens_out[i] = -first_diff(mom, at)
        spread = []
        for n, planes in enumerate((mom, fuel)):
            here = planes[at]
            ya, yb = traded_ref[n * size_x + i], relayed_ref[n * size_x + i]
            tall = jnp.concatenate([jnp.where(odd_y, ya, yb), here, jnp.where(odd_y, yb, ya)], axis=0)
            edge = halo[n][i * size_y : (i + 1) * size_y]

            def along_z(offset):
                if offset == 0:
                    return here
                if offset > 0:
                    return pltpu.roll(jnp.where(lane < offset, edge, here), size_z - offset, 1)
                return pltpu.roll(jnp.where(lane >= size_z + offset, edge, here), -offset, 1)

            spread.append(
                second_diff(lambda o: planes[at + o])
                + second_diff(lambda o: tall[4 + o : 4 + o + size_y])
                + second_diff(along_z)
            )
        mom_out[i] = -first_diff(mom_flux, at) + VISCOSITY * spread[0] + dens[at] * force_ref[i]
        fuel_out[i] = (
            -first_diff(fuel_flux, at) + DIFFUSIVITY * spread[1]
            - fuel[at] * jnp.exp(-ACTIVATION * fuel[at] / dens[at])
        )


def final_rates(density, momentum, hydrogen, summed, cos, sin, depth, halos, ncell):
    shape = density.shape
    return pl.pallas_call(
        functools.partial(final_kernel, ncell),
        out_shape=[jax.ShapeDtypeStruct(shape, jnp.float32)] * 3,
        in_specs=[VMEM] * 13,
        out_specs=[VMEM] * 3,
        scratch_shapes=[pltpu.VMEM(shape, jnp.float32)],
        compiler_params=pltpu.CompilerParams(vmem_limit_bytes=16 << 20),
        name="final_rates",
    )(density, momentum, hydrogen, summed, cos, sin, depth, *halos)


def swap(x, axes, shift):
    size = lax.axis_size(axes)
    pairs = [((i + shift) % size, (i + 1 + shift) % size) for i in range(0, size, 2)]
    return lax.ppermute(x, axes, pairs + [(j, i) for i, j in pairs])


def relay(x):
    size = lax.axis_size("gy_0")
    ups = [(2 * i, 2 * ((i + 1) % size)) for i in range(size)]
    downs = [(2 * i + 1, 2 * ((i - 1) % size) + 1) for i in range(size)]
    return lax.ppermute(x, GY, ups + downs)


def exchange(x, axes):
    return lax.all_to_all(x, axes, 0, 0, tiled=True)


def per_device(density, momentum, hydrogen, forced_modes):
    size_x, size_y, size_z = density.shape
    full = (
        size_x * lax.axis_size(GX),
        size_y * lax.axis_size(GY),
        size_z * lax.axis_size(GZ),
    )
    first, second = lax.axis_size(FIRST_GROUP), lax.axis_size(SECOND_GROUP)
    part, cos, sin, depth, xa, xb, sides, za, zb = partial_sums(
        density, momentum, hydrogen, forced_modes.T, full, first
    )
    za, zb = swap(za, RING, 0), swap(zb, RING, 1)
    part = exchange(part, FIRST_GROUP)
    sides = packed(sides, zb)
    traded = swap(sides, ("gy_1",), 0)
    part = summed_copies(part, second)
    part = exchange(part, SECOND_GROUP)
    xa, xb = swap(xa, GX, 0), swap(xb, GX, 1)
    relayed = relay(traded[2 * size_x : 4 * size_x])
    rates = final_rates(
        density, momentum, hydrogen, part, cos, sin, depth,
        (xa, xb, traded, relayed, za, zb), float(full[0] * full[1] * full[2]),
    )
    return tuple(rates)


def solution(mesh):
    split = Mesh(
        mesh.devices.reshape(8, 2, 4, 2, mesh.shape["gz"]), ("gx_0", "gx_1", "gy_0", "gy_1", "gz")
    )
    field = P(GX, GY, "gz")
    return jax.shard_map(
        per_device, mesh=split, in_specs=(field, field, field, P()),
        out_specs=(field, field, field), check_vma=False,
    )
```

```python
import functools

import jax
import jax.numpy as jnp
from jax import lax
from jax.experimental import pallas as pl
from jax.experimental.pallas import tpu as pltpu
from jax.sharding import Mesh
from jax.sharding import PartitionSpec as P


GX = ("gx_0", "gx_1")
GY = ("gy_0", "gy_1")
GZ = ("gz",)
FIRST_GROUP = ("gx_1", "gy_1", "gz")
RING = ("gy_1", "gz")
SECOND_GROUP = ("gx_0", "gy_0")

FIRST_COEFFS = (0.8, -0.2, 4.0 / 105.0, -1.0 / 280.0)
SECOND_COEFFS = (1.6, -0.2, 8.0 / 315.0, -1.0 / 560.0)
CENTRE_COEFF = -205.0 / 72.0
VISCOSITY = 0.3
DIFFUSIVITY = 1.5
FORCE_POWER = 0.3
ENERGY_EPS = 1e-06
ACTIVATION = 2.0
HIGHEST = lax.Precision.HIGHEST
LANES = 128
VMEM = pl.BlockSpec(memory_space=pltpu.VMEM)


def odd(axis):
    return lax.rem(lax.axis_index(axis), 2) == 1


def angles(wave, start, step, count, total):
    index = lax.broadcasted_iota(jnp.int32, (count, LANES), 0)
    position = (start + step * index).astype(jnp.float32)
    phase = wave * position
    phase = phase - total * jnp.round(phase * (1.0 / total))
    return (2.0 * jnp.pi / total) * phase


def partial_kernel(
    full, copies, dens_hbm, mom_hbm, fuel_hbm, modes_hbm,
    part_ref, cos_ref, sin_ref, depth_ref,
    xlo_ref, xhi_ref, sides_ref, za_ref, zb_ref,
    dens_ref, mom_ref, fuel_ref, modes_ref, sems,
):
    size_x, size_y, size_z = mom_ref.shape
    rows = size_x * size_y
    half = 4
    loads = [
        pltpu.make_async_copy(src, dst, sems.at[n])
        for n, (src, dst) in enumerate(
            ((modes_hbm, modes_ref), (mom_hbm, mom_ref), (dens_hbm, dens_ref), (fuel_hbm, fuel_ref))
        )
    ]
    for load in loads:
        load.start()
    loads[0].wait()
    modes = modes_ref[...].astype(jnp.float32)
    spare = jnp.zeros((1, LANES - modes.shape[1]), jnp.float32)
    wave_x, wave_y, wave_z = (jnp.concatenate([modes[n : n + 1], spare], axis=1) for n in range(3))
    base_x = (lax.axis_index("gx_0") * 2 + lax.axis_index("gx_1")) * size_x
    base_y = (lax.axis_index("gy_0") * 2 + lax.axis_index("gy_1")) * size_y
    base_z = lax.axis_index("gz") * size_z
    fine = size_z // 8
    angle = jnp.concatenate(
        [
            angles(wave_x, base_x, 1, size_x, full[0]),
            angles(wave_y, base_y, 1, size_y, full[1]),
            angles(wave_z, base_z, fine, 8, full[2]),
            angles(wave_z, 0, 1, fine, full[2]),
        ],
        axis=0,
    )
    cos, sin = jnp.cos(angle), jnp.sin(angle)
    at_y, at_z, at_f = size_x, size_x + size_y, size_x + size_y + 8
    cy, sy = cos[at_y:at_z], sin[at_y:at_z]
    live = lax.broadcasted_iota(jnp.int32, (1, LANES), 1) < modes.shape[1]
    cf = jnp.where(live, cos[at_f:], 0.0)
    sf = jnp.where(live, sin[at_f:], 0.0)
    for n in range(size_x):
        cx, sx = cos[n : n + 1], sin[n : n + 1]
        cos_ref[n] = cx * cy - sx * sy
        sin_ref[n] = sx * cy + cx * sy
    for n in range(8):
        cz, sz = cos[at_z + n : at_z + n + 1], sin[at_z + n : at_z + n + 1]
        depth_ref[n * fine : (n + 1) * fine, 0:LANES] = cz * cf - sz * sf
        depth_ref[n * fine : (n + 1) * fine, LANES:] = sz * cf + cz * sf
    loads[1].wait()
    loads[2].wait()
    velocity = (mom_ref[...] / dens_ref[...]).reshape(rows, size_z)
    along = jnp.dot(velocity, depth_ref[...], precision=HIGHEST, preferred_element_type=jnp.float32)
    real, imag = along[:, 0:LANES], along[:, LANES:]
    cos_xy = cos_ref[...].reshape(rows, LANES)
    sin_xy = sin_ref[...].reshape(rows, LANES)
    part_cos = jnp.sum(cos_xy * real - sin_xy * imag, axis=0, keepdims=True)
    part_sin = jnp.sum(sin_xy * real + cos_xy * imag, axis=0, keepdims=True)
    both = jnp.concatenate([part_cos, part_sin], axis=0)
    part_ref[...] = jnp.broadcast_to(both[None], (copies, 2, LANES))
    loads[3].wait()
    odd_y, odd_z = odd("gy_1"), odd("gz")
    for n, ref in enumerate((dens_ref, mom_ref, fuel_ref)):
        xlo_ref[n] = ref[0:half]
        xhi_ref[n] = ref[size_x - half : size_x]
    for n, ref in enumerate((mom_ref, fuel_ref)):
        low, high = ref[:, 0:half, :], ref[:, size_y - half : size_y, :]
        sides_ref[n * size_x : (n + 1) * size_x] = jnp.where(odd_y, low, high)
        sides_ref[(n + 2) * size_x : (n + 3) * size_x] = jnp.where(odd_y, high, low)
    turned = [ref[...].reshape(rows, size_z).T for ref in (mom_ref, fuel_ref)]
    low = jnp.concatenate([t[0:half] for t in turned], axis=0)
    high = jnp.concatenate([t[size_z - half : size_z] for t in turned], axis=0)
    za_ref[...] = jnp.where(odd_z, low, high)
    zb_ref[...] = jnp.where(odd_z, high, low)


def partial_sums(density, momentum, hydrogen, modes, full, copies):
    size_x, size_y, size_z = density.shape
    f32 = jnp.float32
    shapes = (
        (copies, 2, LANES),
        (size_x, size_y, LANES),
        (size_x, size_y, LANES),
        (size_z, 2 * LANES),
        (3, 4, size_y, size_z),
        (3, 4, size_y, size_z),
        (4 * size_x, 4, size_z),
        (8, size_x * size_y),
        (8, size_x * size_y),
    )
    density, momentum, hydrogen, modes = (
        pltpu.with_memory_space_constraint(f, pltpu.HBM) for f in (density, momentum, hydrogen, modes)
    )
    return pl.pallas_call(
        functools.partial(partial_kernel, full, copies),
        out_shape=[jax.ShapeDtypeStruct(s, f32) for s in shapes],
        in_specs=[pl.BlockSpec(memory_space=pltpu.HBM)] * 4,
        out_specs=[VMEM] * len(shapes),
        scratch_shapes=[pltpu.VMEM(density.shape, f32)] * 3
        + [pltpu.VMEM(modes.shape, modes.dtype), pltpu.SemaphoreType.DMA((4,))],
        compiler_params=pltpu.CompilerParams(vmem_limit_bytes=16 << 20),
        name="partial_sums",
    )(density, momentum, hydrogen, modes)


def spread_kernel(parts_ref, out_ref):
    out_ref[...] = jnp.broadcast_to(jnp.sum(parts_ref[...], axis=0, keepdims=True), out_ref.shape)


def summed_copies(parts, copies):
    return pl.pallas_call(
        spread_kernel,
        out_shape=jax.ShapeDtypeStruct((copies,) + parts.shape[1:], jnp.float32),
        in_specs=[VMEM],
        out_specs=VMEM,
        compiler_params=pltpu.CompilerParams(vmem_limit_bytes=4 << 20),
        name="summed_copies",
    )(parts)


def pack_kernel(sides_ref, depth_ref, out_ref):
    count = sides_ref.shape[0]
    out_ref[0:count] = sides_ref[...]
    out_ref[count] = depth_ref[0:4]
    out_ref[count + 1] = depth_ref[4:8]


def packed(sides, depth):
    return pl.pallas_call(
        pack_kernel,
        out_shape=jax.ShapeDtypeStruct((sides.shape[0] + 2,) + sides.shape[1:], jnp.float32),
        in_specs=[VMEM] * 2,
        out_specs=VMEM,
        compiler_params=pltpu.CompilerParams(vmem_limit_bytes=4 << 20),
        name="packed",
    )(sides, depth)


def first_diff(planes, at):
    total = None
    for offset, weight in enumerate(FIRST_COEFFS, 1):
        term = weight * (planes[at + offset] - planes[at - offset])
        total = term if total is None else total + term
    return total


def second_diff(pick):
    total = CENTRE_COEFF * pick(0)
    for offset, weight in enumerate(SECOND_COEFFS, 1):
        total = total + weight * (pick(offset) + pick(-offset))
    return total


def final_kernel(
    ncell, dens_ref, mom_ref, fuel_ref, summed_ref, cos_ref, sin_ref, depth_ref,
    xbefore_ref, xafter_ref, traded_ref, relayed_ref, za_ref, zb_ref,
    dens_out, mom_out, fuel_out, force_ref,
):
    size_x, size_y, size_z = mom_ref.shape
    rows = size_x * size_y
    total = jnp.sum(summed_ref[...], axis=0) * (1.0 / ncell)
    energy = jnp.sum(total * total)
    scaled = total * (2.0 * FORCE_POWER / (energy + ENERGY_EPS))
    coef_cos, coef_sin = scaled[0:1], scaled[1:2]
    cos_xy = cos_ref[...].reshape(rows, LANES)
    sin_xy = sin_ref[...].reshape(rows, LANES)
    side = jnp.concatenate(
        [coef_cos * cos_xy + coef_sin * sin_xy, coef_sin * cos_xy - coef_cos * sin_xy], axis=1
    )
    force_ref[...] = lax.dot_general(
        side, depth_ref[...], (((1,), (1,)), ((), ())), precision=HIGHEST,
        preferred_element_type=jnp.float32,
    ).reshape(size_x, size_y, size_z)
    gap = jnp.zeros((56, rows), jnp.float32)
    odd_y, odd_z = odd("gy_1"), odd("gz")
    place = lax.axis_index("gz")
    at_end = jnp.logical_or(place == 0, place == lax.axis_size("gz") - 1)
    za, zb = za_ref[...], zb_ref[...]
    swapped = jnp.concatenate([traded_ref[4 * size_x], traded_ref[4 * size_x + 1]], axis=0)
    zb = jnp.where(at_end, swapped, zb)
    before = jnp.where(odd_z, za, zb)
    after = jnp.where(odd_z, zb, za)
    turned = jnp.concatenate(
        [after[0:4], gap, before[4:8], after[4:8], gap, before[0:4]], axis=0
    ).T
    halo = [turned, pltpu.roll(turned, 64, 1)]
    lane = lax.broadcasted_iota(jnp.int32, (1, size_z), 1)
    dens, mom, fuel = (
        [xbefore_ref[n, i] for i in range(4)] + [ref[i] for i in range(size_x)] + [xafter_ref[n, i] for i in range(4)]
        for n, ref in enumerate((dens_ref, mom_ref, fuel_ref))
    )
    vel = [m / d for m, d in zip(mom, dens)]
    mom_flux = [m * v + d for m, v, d in zip(mom, vel, dens)]
    fuel_flux = [f * v for f, v in zip(fuel, vel)]
    for i in range(size_x):
        at = i + 4
        dens_out[i] = -first_diff(mom, at)
        spread = []
        for n, planes in enumerate((mom, fuel)):
            here = planes[at]
            ya, yb = traded_ref[n * size_x + i], relayed_ref[n * size_x + i]
            tall = jnp.concatenate([jnp.where(odd_y, ya, yb), here, jnp.where(odd_y, yb, ya)], axis=0)
            edge = halo[n][i * size_y : (i + 1) * size_y]

            def along_z(offset):
                if offset == 0:
                    return here
                if offset > 0:
                    return pltpu.roll(jnp.where(lane < offset, edge, here), size_z - offset, 1)
                return pltpu.roll(jnp.where(lane >= size_z + offset, edge, here), -offset, 1)

            spread.append(
                second_diff(lambda o: planes[at + o])
                + second_diff(lambda o: tall[4 + o : 4 + o + size_y])
                + second_diff(along_z)
            )
        mom_out[i] = -first_diff(mom_flux, at) + VISCOSITY * spread[0] + dens[at] * force_ref[i]
        fuel_out[i] = (
            -first_diff(fuel_flux, at) + DIFFUSIVITY * spread[1]
            - fuel[at] * jnp.exp(-ACTIVATION * fuel[at] / dens[at])
        )


def final_rates(density, momentum, hydrogen, summed, cos, sin, depth, halos, ncell):
    shape = density.shape
    return pl.pallas_call(
        functools.partial(final_kernel, ncell),
        out_shape=[jax.ShapeDtypeStruct(shape, jnp.float32)] * 3,
        in_specs=[VMEM] * 13,
        out_specs=[VMEM] * 3,
        scratch_shapes=[pltpu.VMEM(shape, jnp.float32)],
        compiler_params=pltpu.CompilerParams(vmem_limit_bytes=16 << 20),
        name="final_rates",
    )(density, momentum, hydrogen, summed, cos, sin, depth, *halos)


def shift(x, axes, by):
    size = lax.axis_size(axes)
    return lax.ppermute(x, axes, [(i, (i + by) % size) for i in range(size)])


def swap(x, axes, shift):
    size = lax.axis_size(axes)
    pairs = [((i + shift) % size, (i + 1 + shift) % size) for i in range(0, size, 2)]
    return lax.ppermute(x, axes, pairs + [(j, i) for i, j in pairs])


def relay(x):
    size = lax.axis_size("gy_0")
    ups = [(2 * i, 2 * ((i + 1) % size)) for i in range(size)]
    downs = [(2 * i + 1, 2 * ((i - 1) % size) + 1) for i in range(size)]
    return lax.ppermute(x, GY, ups + downs)


def exchange(x, axes):
    return lax.all_to_all(x, axes, 0, 0, tiled=True)


def per_device(density, momentum, hydrogen, forced_modes):
    size_x, size_y, size_z = density.shape
    full = (
        size_x * lax.axis_size(GX),
        size_y * lax.axis_size(GY),
        size_z * lax.axis_size(GZ),
    )
    first, second = lax.axis_size(FIRST_GROUP), lax.axis_size(SECOND_GROUP)
    part, cos, sin, depth, xlo, xhi, sides, za, zb = partial_sums(
        density, momentum, hydrogen, forced_modes.T, full, first
    )
    zb = swap(zb, RING, 1)
    part = exchange(part, FIRST_GROUP)
    sides = packed(sides, zb)
    traded = swap(sides, ("gy_1",), 0)
    part = summed_copies(part, second)
    part = exchange(part, SECOND_GROUP)
    xbefore, xafter = shift(xhi, GX, 1), shift(xlo, GX, -1)
    za = swap(za, GZ, 0)
    relayed = relay(traded[2 * size_x : 4 * size_x])
    rates = final_rates(
        density, momentum, hydrogen, part, cos, sin, depth,
        (xbefore, xafter, traded, relayed, za, zb), float(full[0] * full[1] * full[2]),
    )
    return tuple(rates)


def solution(mesh):
    split = Mesh(
        mesh.devices.reshape(8, 2, 4, 2, mesh.shape["gz"]), ("gx_0", "gx_1", "gy_0", "gy_1", "gz")
    )
    field = P(GX, GY, "gz")
    return jax.shard_map(
        per_device, mesh=split, in_specs=(field, field, field, P()),
        out_specs=(field, field, field), check_vma=False,
    )
```

```python
import functools

import jax
import jax.numpy as jnp
from jax import lax
from jax.experimental import pallas as pl
from jax.experimental.pallas import tpu as pltpu
from jax.sharding import Mesh
from jax.sharding import PartitionSpec as P


GX = ("gx_0", "gx_1")
GY = ("gy_0", "gy_1")
GZ = ("gz",)
FIRST_GROUP = ("gx_0", "gy_0")
RING = ("gy_1", "gz")
SECOND_GROUP = ("gx_1", "gy_1", "gz")

FIRST_COEFFS = (0.8, -0.2, 4.0 / 105.0, -1.0 / 280.0)
SECOND_COEFFS = (1.6, -0.2, 8.0 / 315.0, -1.0 / 560.0)
CENTRE_COEFF = -205.0 / 72.0
VISCOSITY = 0.3
DIFFUSIVITY = 1.5
FORCE_POWER = 0.3
ENERGY_EPS = 1e-06
ACTIVATION = 2.0
HIGHEST = lax.Precision.HIGHEST
LANES = 128
VMEM = pl.BlockSpec(memory_space=pltpu.VMEM)


def odd(axis):
    return lax.rem(lax.axis_index(axis), 2) == 1


def angles(wave, start, step, count, total):
    index = lax.broadcasted_iota(jnp.int32, (count, LANES), 0)
    position = (start + step * index).astype(jnp.float32)
    phase = wave * position
    phase = phase - total * jnp.round(phase * (1.0 / total))
    return (2.0 * jnp.pi / total) * phase


def partial_kernel(
    full, copies, dens_hbm, mom_hbm, fuel_hbm, modes_hbm,
    part_ref, cos_ref, sin_ref, depth_ref,
    xlo_ref, xhi_ref, sides_ref, za_ref, zb_ref,
    dens_ref, mom_ref, fuel_ref, modes_ref, sems,
):
    size_x, size_y, size_z = mom_ref.shape
    rows = size_x * size_y
    half = 4
    loads = [
        pltpu.make_async_copy(src, dst, sems.at[n])
        for n, (src, dst) in enumerate(
            ((modes_hbm, modes_ref), (mom_hbm, mom_ref), (dens_hbm, dens_ref), (fuel_hbm, fuel_ref))
        )
    ]
    for load in loads:
        load.start()
    loads[0].wait()
    modes = modes_ref[...].astype(jnp.float32)
    spare = jnp.zeros((1, LANES - modes.shape[1]), jnp.float32)
    wave_x, wave_y, wave_z = (jnp.concatenate([modes[n : n + 1], spare], axis=1) for n in range(3))
    base_x = (lax.axis_index("gx_0") * 2 + lax.axis_index("gx_1")) * size_x
    base_y = (lax.axis_index("gy_0") * 2 + lax.axis_index("gy_1")) * size_y
    base_z = lax.axis_index("gz") * size_z
    fine = size_z // 8
    angle = jnp.concatenate(
        [
            angles(wave_x, base_x, 1, size_x, full[0]),
            angles(wave_y, base_y, 1, size_y, full[1]),
            angles(wave_z, base_z, fine, 8, full[2]),
            angles(wave_z, 0, 1, fine, full[2]),
        ],
        axis=0,
    )
    cos, sin = jnp.cos(angle), jnp.sin(angle)
    at_y, at_z, at_f = size_x, size_x + size_y, size_x + size_y + 8
    cy, sy = cos[at_y:at_z], sin[at_y:at_z]
    live = lax.broadcasted_iota(jnp.int32, (1, LANES), 1) < modes.shape[1]
    cf = jnp.where(live, cos[at_f:], 0.0)
    sf = jnp.where(live, sin[at_f:], 0.0)
    for n in range(size_x):
        cx, sx = cos[n : n + 1], sin[n : n + 1]
        cos_ref[n] = cx * cy - sx * sy
        sin_ref[n] = sx * cy + cx * sy
    for n in range(8):
        cz, sz = cos[at_z + n : at_z + n + 1], sin[at_z + n : at_z + n + 1]
        depth_ref[n * fine : (n + 1) * fine, 0:LANES] = cz * cf - sz * sf
        depth_ref[n * fine : (n + 1) * fine, LANES:] = sz * cf + cz * sf
    loads[1].wait()
    loads[2].wait()
    velocity = (mom_ref[...] / dens_ref[...]).reshape(rows, size_z)
    along = jnp.dot(velocity, depth_ref[...], precision=HIGHEST, preferred_element_type=jnp.float32)
    real, imag = along[:, 0:LANES], along[:, LANES:]
    cos_xy = cos_ref[...].reshape(rows, LANES)
    sin_xy = sin_ref[...].reshape(rows, LANES)
    part_cos = jnp.sum(cos_xy * real - sin_xy * imag, axis=0, keepdims=True)
    part_sin = jnp.sum(sin_xy * real + cos_xy * imag, axis=0, keepdims=True)
    both = jnp.concatenate([part_cos, part_sin], axis=0)
    part_ref[...] = jnp.broadcast_to(both[None], (copies, 2, LANES))
    loads[3].wait()
    odd_y, odd_z = odd("gy_1"), odd("gz")
    for n, ref in enumerate((dens_ref, mom_ref, fuel_ref)):
        xlo_ref[n] = ref[0:half]
        xhi_ref[n] = ref[size_x - half : size_x]
    for n, ref in enumerate((mom_ref, fuel_ref)):
        low, high = ref[:, 0:half, :], ref[:, size_y - half : size_y, :]
        sides_ref[n * size_x : (n + 1) * size_x] = jnp.where(odd_y, low, high)
        sides_ref[(n + 2) * size_x : (n + 3) * size_x] = jnp.where(odd_y, high, low)
    turned = [ref[...].reshape(rows, size_z).T for ref in (mom_ref, fuel_ref)]
    low = jnp.concatenate([t[0:half] for t in turned], axis=0)
    high = jnp.concatenate([t[size_z - half : size_z] for t in turned], axis=0)
    za_ref[...] = jnp.where(odd_z, low, high)
    edge = jnp.where(odd_z, high, low)
    zb_ref[...] = edge
    sides_ref[4 * size_x] = edge[0:4]
    sides_ref[4 * size_x + 1] = edge[4:8]


def partial_sums(density, momentum, hydrogen, modes, full, copies):
    size_x, size_y, size_z = density.shape
    f32 = jnp.float32
    shapes = (
        (copies, 2, LANES),
        (size_x, size_y, LANES),
        (size_x, size_y, LANES),
        (size_z, 2 * LANES),
        (3, 4, size_y, size_z),
        (3, 4, size_y, size_z),
        (4 * size_x + 2, 4, size_z),
        (8, size_x * size_y),
        (8, size_x * size_y),
    )
    density, momentum, hydrogen, modes = (
        pltpu.with_memory_space_constraint(f, pltpu.HBM) for f in (density, momentum, hydrogen, modes)
    )
    return pl.pallas_call(
        functools.partial(partial_kernel, full, copies),
        out_shape=[jax.ShapeDtypeStruct(s, f32) for s in shapes],
        in_specs=[pl.BlockSpec(memory_space=pltpu.HBM)] * 4,
        out_specs=[VMEM] * len(shapes),
        scratch_shapes=[pltpu.VMEM(density.shape, f32)] * 3
        + [pltpu.VMEM(modes.shape, modes.dtype), pltpu.SemaphoreType.DMA((4,))],
        compiler_params=pltpu.CompilerParams(vmem_limit_bytes=16 << 20),
        name="partial_sums",
    )(density, momentum, hydrogen, modes)


def spread_kernel(parts_ref, out_ref):
    out_ref[...] = jnp.broadcast_to(jnp.sum(parts_ref[...], axis=0, keepdims=True), out_ref.shape)


def summed_copies(parts, copies):
    return pl.pallas_call(
        spread_kernel,
        out_shape=jax.ShapeDtypeStruct((copies,) + parts.shape[1:], jnp.float32),
        in_specs=[VMEM],
        out_specs=VMEM,
        compiler_params=pltpu.CompilerParams(vmem_limit_bytes=4 << 20),
        name="summed_copies",
    )(parts)


def forward_kernel(traded_ref, edge_ref, relay_ref, hop_ref):
    count = relay_ref.shape[0]
    relay_ref[...] = traded_ref[count : 2 * count]
    place = lax.axis_index("gz")
    at_end = jnp.logical_or(place == 0, place == lax.axis_size("gz") - 1)
    partners = jnp.concatenate([traded_ref[2 * count], traded_ref[2 * count + 1]], axis=0)
    hop_ref[...] = jnp.where(at_end, partners, edge_ref[...])


def forwarded(traded, edge):
    count = (traded.shape[0] - 2) // 2
    return pl.pallas_call(
        forward_kernel,
        out_shape=[
            jax.ShapeDtypeStruct((count,) + traded.shape[1:], jnp.float32),
            jax.ShapeDtypeStruct(edge.shape, jnp.float32),
        ],
        in_specs=[VMEM] * 2,
        out_specs=[VMEM] * 2,
        compiler_params=pltpu.CompilerParams(vmem_limit_bytes=4 << 20),
        name="forwarded",
    )(traded, edge)


def first_diff(planes, at):
    total = None
    for offset, weight in enumerate(FIRST_COEFFS, 1):
        term = weight * (planes[at + offset] - planes[at - offset])
        total = term if total is None else total + term
    return total


def second_diff(pick):
    total = CENTRE_COEFF * pick(0)
    for offset, weight in enumerate(SECOND_COEFFS, 1):
        total = total + weight * (pick(offset) + pick(-offset))
    return total


def final_kernel(
    ncell, dens_ref, mom_ref, fuel_ref, summed_ref, cos_ref, sin_ref, depth_ref,
    xbefore_ref, xafter_ref, traded_ref, relayed_ref, za_ref, zb_ref,
    dens_out, mom_out, fuel_out, force_ref,
):
    size_x, size_y, size_z = mom_ref.shape
    rows = size_x * size_y
    total = jnp.sum(summed_ref[...], axis=0) * (1.0 / ncell)
    energy = jnp.sum(total * total)
    scaled = total * (2.0 * FORCE_POWER / (energy + ENERGY_EPS))
    coef_cos, coef_sin = scaled[0:1], scaled[1:2]
    cos_xy = cos_ref[...].reshape(rows, LANES)
    sin_xy = sin_ref[...].reshape(rows, LANES)
    side = jnp.concatenate(
        [coef_cos * cos_xy + coef_sin * sin_xy, coef_sin * cos_xy - coef_cos * sin_xy], axis=1
    )
    force_ref[...] = lax.dot_general(
        side, depth_ref[...], (((1,), (1,)), ((), ())), precision=HIGHEST,
        preferred_element_type=jnp.float32,
    ).reshape(size_x, size_y, size_z)
    gap = jnp.zeros((56, rows), jnp.float32)
    odd_y, odd_z = odd("gy_1"), odd("gz")
    za, zb = za_ref[...], zb_ref[...]
    before = jnp.where(odd_z, za, zb)
    after = jnp.where(odd_z, zb, za)
    turned = jnp.concatenate(
        [after[0:4], gap, before[4:8], after[4:8], gap, before[0:4]], axis=0
    ).T
    halo = [turned, pltpu.roll(turned, 64, 1)]
    lane = lax.broadcasted_iota(jnp.int32, (1, size_z), 1)
    dens, mom, fuel = (
        [xbefore_ref[n, i] for i in range(4)] + [ref[i] for i in range(size_x)] + [xafter_ref[n, i] for i in range(4)]
        for n, ref in enumerate((dens_ref, mom_ref, fuel_ref))
    )
    vel = [m / d for m, d in zip(mom, dens)]
    mom_flux = [m * v + d for m, v, d in zip(mom, vel, dens)]
    fuel_flux = [f * v for f, v in zip(fuel, vel)]
    for i in range(size_x):
        at = i + 4
        dens_out[i] = -first_diff(mom, at)
        spread = []
        for n, planes in enumerate((mom, fuel)):
            here = planes[at]
            ya, yb = traded_ref[n * size_x + i], relayed_ref[n * size_x + i]
            tall = jnp.concatenate([jnp.where(odd_y, ya, yb), here, jnp.where(odd_y, yb, ya)], axis=0)
            edge = halo[n][i * size_y : (i + 1) * size_y]

            def along_z(offset):
                if offset == 0:
                    return here
                if offset > 0:
                    return pltpu.roll(jnp.where(lane < offset, edge, here), size_z - offset, 1)
                return pltpu.roll(jnp.where(lane >= size_z + offset, edge, here), -offset, 1)

            spread.append(
                second_diff(lambda o: planes[at + o])
                + second_diff(lambda o: tall[4 + o : 4 + o + size_y])
                + second_diff(along_z)
            )
        mom_out[i] = -first_diff(mom_flux, at) + VISCOSITY * spread[0] + dens[at] * force_ref[i]
        fuel_out[i] = (
            -first_diff(fuel_flux, at) + DIFFUSIVITY * spread[1]
            - fuel[at] * jnp.exp(-ACTIVATION * fuel[at] / dens[at])
        )


def final_rates(density, momentum, hydrogen, summed, cos, sin, depth, halos, ncell):
    shape = density.shape
    return pl.pallas_call(
        functools.partial(final_kernel, ncell),
        out_shape=[jax.ShapeDtypeStruct(shape, jnp.float32)] * 3,
        in_specs=[VMEM] * 13,
        out_specs=[VMEM] * 3,
        scratch_shapes=[pltpu.VMEM(shape, jnp.float32)],
        compiler_params=pltpu.CompilerParams(vmem_limit_bytes=16 << 20),
        name="final_rates",
    )(density, momentum, hydrogen, summed, cos, sin, depth, *halos)


def shift(x, axes, by):
    size = lax.axis_size(axes)
    return lax.ppermute(x, axes, [(i, (i + by) % size) for i in range(size)])


def swap(x, axes, shift):
    size = lax.axis_size(axes)
    pairs = [((i + shift) % size, (i + 1 + shift) % size) for i in range(0, size, 2)]
    return lax.ppermute(x, axes, pairs + [(j, i) for i, j in pairs])


def relay(x):
    size = lax.axis_size("gy_0")
    ups = [(2 * i, 2 * ((i + 1) % size)) for i in range(size)]
    downs = [(2 * i + 1, 2 * ((i - 1) % size) + 1) for i in range(size)]
    return lax.ppermute(x, GY, ups + downs)


def exchange(x, axes):
    return lax.all_to_all(x, axes, 0, 0, tiled=True)


def per_device(density, momentum, hydrogen, forced_modes):
    size_x, size_y, size_z = density.shape
    full = (
        size_x * lax.axis_size(GX),
        size_y * lax.axis_size(GY),
        size_z * lax.axis_size(GZ),
    )
    first, second = lax.axis_size(FIRST_GROUP), lax.axis_size(SECOND_GROUP)
    part, cos, sin, depth, xlo, xhi, sides, za, zb = partial_sums(
        density, momentum, hydrogen, forced_modes.T, full, first
    )
    traded = swap(sides, ("gy_1",), 0)
    part = exchange(part, FIRST_GROUP)
    xbefore, xafter = shift(xhi, GX, 1), shift(xlo, GX, -1)
    za = swap(za, GZ, 0)
    part = summed_copies(part, second)
    part = exchange(part, SECOND_GROUP)
    relayed, zb = forwarded(traded, zb)
    relayed = relay(relayed)
    zb = swap(zb, RING, 1)
    rates = final_rates(
        density, momentum, hydrogen, part, cos, sin, depth,
        (xbefore, xafter, traded, relayed, za, zb), float(full[0] * full[1] * full[2]),
    )
    return tuple(rates)


def solution(mesh):
    split = Mesh(
        mesh.devices.reshape(8, 2, 4, 2, mesh.shape["gz"]), ("gx_0", "gx_1", "gy_0", "gy_1", "gz")
    )
    field = P(GX, GY, "gz")
    return jax.shard_map(
        per_device, mesh=split, in_specs=(field, field, field, P()),
        out_specs=(field, field, field), check_vma=False,
    )
```

```python
import functools

import jax
import jax.numpy as jnp
from jax import lax
from jax.experimental import pallas as pl
from jax.experimental.pallas import tpu as pltpu
from jax.sharding import Mesh
from jax.sharding import PartitionSpec as P


GX = ("gx_0", "gx_1")
GY = ("gy_0", "gy_1")
GZ = ("gz",)
FIRST_GROUP = ("gy_1", "gz")
SECOND_GROUP = ("gx_0", "gx_1", "gy_0")

FIRST_COEFFS = (0.8, -0.2, 4.0 / 105.0, -1.0 / 280.0)
SECOND_COEFFS = (1.6, -0.2, 8.0 / 315.0, -1.0 / 560.0)
CENTRE_COEFF = -205.0 / 72.0
VISCOSITY = 0.3
DIFFUSIVITY = 1.5
FORCE_POWER = 0.3
ENERGY_EPS = 1e-06
ACTIVATION = 2.0
HIGHEST = lax.Precision.HIGHEST
LANES = 128
VMEM = pl.BlockSpec(memory_space=pltpu.VMEM)


def odd(axis):
    return lax.rem(lax.axis_index(axis), 2) == 1


def depth_places():
    place, count = lax.axis_index("gz"), lax.axis_size("gz")
    base = lax.axis_index("gy_1") * count
    return base + lax.rem(place + 1, count), base + lax.rem(place + count - 1, count)


def angles(wave, start, step, count, total):
    index = lax.broadcasted_iota(jnp.int32, (count, LANES), 0)
    position = (start + step * index).astype(jnp.float32)
    phase = wave * position
    phase = phase - total * jnp.round(phase * (1.0 / total))
    return (2.0 * jnp.pi / total) * phase


def partial_kernel(
    full, copies, dens_hbm, mom_hbm, fuel_hbm, modes_hbm,
    part_ref, cos_ref, sin_ref, depth_ref,
    xlo_ref, xhi_ref, sides_ref,
    dens_ref, mom_ref, fuel_ref, modes_ref, sems,
):
    size_x, size_y, size_z = mom_ref.shape
    rows = size_x * size_y
    half = 4
    loads = [
        pltpu.make_async_copy(src, dst, sems.at[n])
        for n, (src, dst) in enumerate(
            ((modes_hbm, modes_ref), (mom_hbm, mom_ref), (dens_hbm, dens_ref), (fuel_hbm, fuel_ref))
        )
    ]
    for load in loads:
        load.start()
    loads[0].wait()
    modes = modes_ref[...].astype(jnp.float32)
    spare = jnp.zeros((1, LANES - modes.shape[1]), jnp.float32)
    wave_x, wave_y, wave_z = (jnp.concatenate([modes[n : n + 1], spare], axis=1) for n in range(3))
    base_x = (lax.axis_index("gx_0") * 2 + lax.axis_index("gx_1")) * size_x
    base_y = (lax.axis_index("gy_0") * 2 + lax.axis_index("gy_1")) * size_y
    base_z = lax.axis_index("gz") * size_z
    fine = size_z // 8
    angle = jnp.concatenate(
        [
            angles(wave_x, base_x, 1, size_x, full[0]),
            angles(wave_y, base_y, 1, size_y, full[1]),
            angles(wave_z, base_z, fine, 8, full[2]),
            angles(wave_z, 0, 1, fine, full[2]),
        ],
        axis=0,
    )
    cos, sin = jnp.cos(angle), jnp.sin(angle)
    at_y, at_z, at_f = size_x, size_x + size_y, size_x + size_y + 8
    cy, sy = cos[at_y:at_z], sin[at_y:at_z]
    live = lax.broadcasted_iota(jnp.int32, (1, LANES), 1) < modes.shape[1]
    cf = jnp.where(live, cos[at_f:], 0.0)
    sf = jnp.where(live, sin[at_f:], 0.0)
    for n in range(size_x):
        cx, sx = cos[n : n + 1], sin[n : n + 1]
        cos_ref[n] = cx * cy - sx * sy
        sin_ref[n] = sx * cy + cx * sy
    for n in range(8):
        cz, sz = cos[at_z + n : at_z + n + 1], sin[at_z + n : at_z + n + 1]
        depth_ref[n * fine : (n + 1) * fine, 0:LANES] = cz * cf - sz * sf
        depth_ref[n * fine : (n + 1) * fine, LANES:] = sz * cf + cz * sf
    loads[1].wait()
    loads[2].wait()
    velocity = (mom_ref[...] / dens_ref[...]).reshape(rows, size_z)
    along = jnp.dot(velocity, depth_ref[...], precision=HIGHEST, preferred_element_type=jnp.float32)
    real, imag = along[:, 0:LANES], along[:, LANES:]
    cos_xy = cos_ref[...].reshape(rows, LANES)
    sin_xy = sin_ref[...].reshape(rows, LANES)
    part_cos = jnp.sum(cos_xy * real - sin_xy * imag, axis=0, keepdims=True)
    part_sin = jnp.sum(sin_xy * real + cos_xy * imag, axis=0, keepdims=True)
    both = jnp.concatenate([part_cos, part_sin], axis=0)
    part_ref[:, 0] = jnp.broadcast_to(both[None], (copies, 2, LANES))
    loads[3].wait()
    odd_y = odd("gy_1")
    for n, ref in enumerate((dens_ref, mom_ref, fuel_ref)):
        xlo_ref[n] = ref[0:half]
        xhi_ref[n] = ref[size_x - half : size_x]
    for n, ref in enumerate((mom_ref, fuel_ref)):
        low, high = ref[:, 0:half, :], ref[:, size_y - half : size_y, :]
        sides_ref[n * size_x : (n + 1) * size_x] = jnp.where(odd_y, low, high)
        sides_ref[(n + 2) * size_x : (n + 3) * size_x] = jnp.where(odd_y, high, low)
    turned = [ref[...].reshape(rows, size_z).T for ref in (mom_ref, fuel_ref)]
    low = jnp.concatenate([t[0:half] for t in turned], axis=0)
    high = jnp.concatenate([t[size_z - half : size_z] for t in turned], axis=0)
    following, _ = depth_places()
    for n in range(4):
        pair = slice(2 * n, 2 * n + 2)
        part_ref[:, 1 + n] = jnp.broadcast_to(low[pair][None], (copies, 2, LANES))
        part_ref[pl.ds(following, 1), 1 + n] = high[pair][None]


def partial_sums(density, momentum, hydrogen, modes, full, copies):
    size_x, size_y, size_z = density.shape
    f32 = jnp.float32
    shapes = (
        (copies, 5, 2, LANES),
        (size_x, size_y, LANES),
        (size_x, size_y, LANES),
        (size_z, 2 * LANES),
        (3, 4, size_y, size_z),
        (3, 4, size_y, size_z),
        (4 * size_x, 4, size_z),
    )
    density, momentum, hydrogen, modes = (
        pltpu.with_memory_space_constraint(f, pltpu.HBM) for f in (density, momentum, hydrogen, modes)
    )
    return pl.pallas_call(
        functools.partial(partial_kernel, full, copies),
        out_shape=[jax.ShapeDtypeStruct(s, f32) for s in shapes],
        in_specs=[pl.BlockSpec(memory_space=pltpu.HBM)] * 4,
        out_specs=[VMEM] * len(shapes),
        scratch_shapes=[pltpu.VMEM(density.shape, f32)] * 3
        + [pltpu.VMEM(modes.shape, modes.dtype), pltpu.SemaphoreType.DMA((4,))],
        compiler_params=pltpu.CompilerParams(vmem_limit_bytes=16 << 20),
        name="partial_sums",
    )(density, momentum, hydrogen, modes)


def spread_kernel(parts_ref, out_ref, before_ref, after_ref):
    total = jnp.sum(parts_ref[:, 0], axis=0, keepdims=True)
    out_ref[...] = jnp.broadcast_to(total, out_ref.shape)
    following, preceding = depth_places()
    for n in range(4):
        pair = slice(2 * n, 2 * n + 2)
        before_ref[pair] = parts_ref[preceding, 1 + n]
        after_ref[pair] = parts_ref[following, 1 + n]


def summed_copies(parts, copies):
    edge = jax.ShapeDtypeStruct((8, LANES), jnp.float32)
    return pl.pallas_call(
        spread_kernel,
        out_shape=[jax.ShapeDtypeStruct((copies, 2, LANES), jnp.float32), edge, edge],
        in_specs=[VMEM],
        out_specs=[VMEM] * 3,
        compiler_params=pltpu.CompilerParams(vmem_limit_bytes=4 << 20),
        name="summed_copies",
    )(parts)


def first_diff(planes, at):
    total = None
    for offset, weight in enumerate(FIRST_COEFFS, 1):
        term = weight * (planes[at + offset] - planes[at - offset])
        total = term if total is None else total + term
    return total


def second_diff(pick):
    total = CENTRE_COEFF * pick(0)
    for offset, weight in enumerate(SECOND_COEFFS, 1):
        total = total + weight * (pick(offset) + pick(-offset))
    return total


def final_kernel(
    ncell, dens_ref, mom_ref, fuel_ref, summed_ref, cos_ref, sin_ref, depth_ref,
    xbefore_ref, xafter_ref, traded_ref, relayed_ref, zbefore_ref, zafter_ref,
    dens_out, mom_out, fuel_out, force_ref,
):
    size_x, size_y, size_z = mom_ref.shape
    rows = size_x * size_y
    total = jnp.sum(summed_ref[...], axis=0) * (1.0 / ncell)
    energy = jnp.sum(total * total)
    scaled = total * (2.0 * FORCE_POWER / (energy + ENERGY_EPS))
    coef_cos, coef_sin = scaled[0:1], scaled[1:2]
    cos_xy = cos_ref[...].reshape(rows, LANES)
    sin_xy = sin_ref[...].reshape(rows, LANES)
    side = jnp.concatenate(
        [coef_cos * cos_xy + coef_sin * sin_xy, coef_sin * cos_xy - coef_cos * sin_xy], axis=1
    )
    force_ref[...] = lax.dot_general(
        side, depth_ref[...], (((1,), (1,)), ((), ())), precision=HIGHEST,
        preferred_element_type=jnp.float32,
    ).reshape(size_x, size_y, size_z)
    gap = jnp.zeros((56, rows), jnp.float32)
    odd_y = odd("gy_1")
    before, after = zbefore_ref[...], zafter_ref[...]
    turned = jnp.concatenate(
        [after[0:4], gap, before[4:8], after[4:8], gap, before[0:4]], axis=0
    ).T
    halo = [turned, pltpu.roll(turned, 64, 1)]
    lane = lax.broadcasted_iota(jnp.int32, (1, size_z), 1)
    dens, mom, fuel = (
        [xbefore_ref[n, i] for i in range(4)] + [ref[i] for i in range(size_x)] + [xafter_ref[n, i] for i in range(4)]
        for n, ref in enumerate((dens_ref, mom_ref, fuel_ref))
    )
    vel = [m / d for m, d in zip(mom, dens)]
    mom_flux = [m * v + d for m, v, d in zip(mom, vel, dens)]
    fuel_flux = [f * v for f, v in zip(fuel, vel)]
    for i in range(size_x):
        at = i + 4
        dens_out[i] = -first_diff(mom, at)
        spread = []
        for n, planes in enumerate((mom, fuel)):
            here = planes[at]
            ya, yb = traded_ref[n * size_x + i], relayed_ref[n * size_x + i]
            tall = jnp.concatenate([jnp.where(odd_y, ya, yb), here, jnp.where(odd_y, yb, ya)], axis=0)
            edge = halo[n][i * size_y : (i + 1) * size_y]

            def along_z(offset):
                if offset == 0:
                    return here
                if offset > 0:
                    return pltpu.roll(jnp.where(lane < offset, edge, here), size_z - offset, 1)
                return pltpu.roll(jnp.where(lane >= size_z + offset, edge, here), -offset, 1)

            spread.append(
                second_diff(lambda o: planes[at + o])
                + second_diff(lambda o: tall[4 + o : 4 + o + size_y])
                + second_diff(along_z)
            )
        mom_out[i] = -first_diff(mom_flux, at) + VISCOSITY * spread[0] + dens[at] * force_ref[i]
        fuel_out[i] = (
            -first_diff(fuel_flux, at) + DIFFUSIVITY * spread[1]
            - fuel[at] * jnp.exp(-ACTIVATION * fuel[at] / dens[at])
        )


def final_rates(density, momentum, hydrogen, summed, cos, sin, depth, halos, ncell):
    shape = density.shape
    return pl.pallas_call(
        functools.partial(final_kernel, ncell),
        out_shape=[jax.ShapeDtypeStruct(shape, jnp.float32)] * 3,
        in_specs=[VMEM] * 13,
        out_specs=[VMEM] * 3,
        scratch_shapes=[pltpu.VMEM(shape, jnp.float32)],
        compiler_params=pltpu.CompilerParams(vmem_limit_bytes=16 << 20),
        name="final_rates",
    )(density, momentum, hydrogen, summed, cos, sin, depth, *halos)


def shift(x, axes, by):
    size = lax.axis_size(axes)
    return lax.ppermute(x, axes, [(i, (i + by) % size) for i in range(size)])


def swap(x, axes, shift):
    size = lax.axis_size(axes)
    pairs = [((i + shift) % size, (i + 1 + shift) % size) for i in range(0, size, 2)]
    return lax.ppermute(x, axes, pairs + [(j, i) for i, j in pairs])


def relay(x):
    size = lax.axis_size("gy_0")
    ups = [(2 * i, 2 * ((i + 1) % size)) for i in range(size)]
    downs = [(2 * i + 1, 2 * ((i - 1) % size) + 1) for i in range(size)]
    return lax.ppermute(x, GY, ups + downs)


def exchange(x, axes):
    return lax.all_to_all(x, axes, 0, 0, tiled=True)


def per_device(density, momentum, hydrogen, forced_modes):
    size_x, size_y, size_z = density.shape
    full = (
        size_x * lax.axis_size(GX),
        size_y * lax.axis_size(GY),
        size_z * lax.axis_size(GZ),
    )
    first, second = lax.axis_size(FIRST_GROUP), lax.axis_size(SECOND_GROUP)
    part, cos, sin, depth, xlo, xhi, sides = partial_sums(
        density, momentum, hydrogen, forced_modes.T, full, first
    )
    part = exchange(part, FIRST_GROUP)
    traded = swap(sides, ("gy_1",), 0)
    part, zbefore, zafter = summed_copies(part, second)
    part = exchange(part, SECOND_GROUP)
    xbefore, xafter = shift(xhi, GX, 1), shift(xlo, GX, -1)
    relayed = relay(traded[2 * size_x : 4 * size_x])
    rates = final_rates(
        density, momentum, hydrogen, part, cos, sin, depth,
        (xbefore, xafter, traded, relayed, zbefore, zafter), float(full[0] * full[1] * full[2]),
    )
    return tuple(rates)


def solution(mesh):
    split = Mesh(
        mesh.devices.reshape(8, 2, 4, 2, mesh.shape["gz"]), ("gx_0", "gx_1", "gy_0", "gy_1", "gz")
    )
    field = P(GX, GY, "gz")
    return jax.shard_map(
        per_device, mesh=split, in_specs=(field, field, field, P()),
        out_specs=(field, field, field), check_vma=False,
    )
```

```python
import functools

import jax
import jax.numpy as jnp
from jax import lax
from jax.experimental import pallas as pl
from jax.experimental.pallas import tpu as pltpu
from jax.sharding import Mesh
from jax.sharding import PartitionSpec as P


GX = ("gx_0", "gx_1")
GY = ("gy_0", "gy_1")
GZ = ("gz",)
FIRST_GROUP = ("gy_1", "gz")
FIRST_MEMBER = 8
SECOND_GROUP = ("gx_0", "gx_1", "gy_0")

FIRST_COEFFS = (0.8, -0.2, 4.0 / 105.0, -1.0 / 280.0)
SECOND_COEFFS = (1.6, -0.2, 8.0 / 315.0, -1.0 / 560.0)
CENTRE_COEFF = -205.0 / 72.0
VISCOSITY = 0.3
DIFFUSIVITY = 1.5
FORCE_POWER = 0.3
ENERGY_EPS = 1e-06
ACTIVATION = 2.0
HIGHEST = lax.Precision.HIGHEST
LANES = 128
VMEM = pl.BlockSpec(memory_space=pltpu.VMEM)


def odd(axis):
    return lax.rem(lax.axis_index(axis), 2) == 1


def depth_places():
    place, count = lax.axis_index("gz"), lax.axis_size("gz")
    whole = count * lax.axis_size("gy_1")
    base = lax.axis_index("gy_1") * count + whole - FIRST_MEMBER
    return tuple(lax.rem(base + lax.rem(place + by, count), whole) for by in (1, count - 1))


def angles(wave, start, step, count, total):
    index = lax.broadcasted_iota(jnp.int32, (count, LANES), 0)
    position = (start + step * index).astype(jnp.float32)
    phase = wave * position
    phase = phase - total * jnp.round(phase * (1.0 / total))
    return (2.0 * jnp.pi / total) * phase


def partial_kernel(
    full, copies, dens_hbm, mom_hbm, fuel_hbm, modes_hbm,
    part_ref, cos_ref, sin_ref, depth_ref,
    xlo_ref, xhi_ref, sides_ref,
    dens_ref, mom_ref, fuel_ref, modes_ref, sems,
):
    size_x, size_y, size_z = mom_ref.shape
    rows = size_x * size_y
    half = 4
    loads = [
        pltpu.make_async_copy(src, dst, sems.at[n])
        for n, (src, dst) in enumerate(
            ((modes_hbm, modes_ref), (mom_hbm, mom_ref), (dens_hbm, dens_ref), (fuel_hbm, fuel_ref))
        )
    ]
    for load in loads:
        load.start()
    loads[0].wait()
    modes = modes_ref[...].astype(jnp.float32)
    spare = jnp.zeros((1, LANES - modes.shape[1]), jnp.float32)
    wave_x, wave_y, wave_z = (jnp.concatenate([modes[n : n + 1], spare], axis=1) for n in range(3))
    base_x = (lax.axis_index("gx_0") * 2 + lax.axis_index("gx_1")) * size_x
    base_y = (lax.axis_index("gy_0") * 2 + lax.axis_index("gy_1")) * size_y
    base_z = lax.axis_index("gz") * size_z
    fine = size_z // 8
    angle = jnp.concatenate(
        [
            angles(wave_x, base_x, 1, size_x, full[0]),
            angles(wave_y, base_y, 1, size_y, full[1]),
            angles(wave_z, base_z, fine, 8, full[2]),
            angles(wave_z, 0, 1, fine, full[2]),
        ],
        axis=0,
    )
    cos, sin = jnp.cos(angle), jnp.sin(angle)
    at_y, at_z, at_f = size_x, size_x + size_y, size_x + size_y + 8
    cy, sy = cos[at_y:at_z], sin[at_y:at_z]
    live = lax.broadcasted_iota(jnp.int32, (1, LANES), 1) < modes.shape[1]
    cf = jnp.where(live, cos[at_f:], 0.0)
    sf = jnp.where(live, sin[at_f:], 0.0)
    for n in range(size_x):
        cx, sx = cos[n : n + 1], sin[n : n + 1]
        cos_ref[n] = cx * cy - sx * sy
        sin_ref[n] = sx * cy + cx * sy
    for n in range(8):
        cz, sz = cos[at_z + n : at_z + n + 1], sin[at_z + n : at_z + n + 1]
        depth_ref[n * fine : (n + 1) * fine, 0:LANES] = cz * cf - sz * sf
        depth_ref[n * fine : (n + 1) * fine, LANES:] = sz * cf + cz * sf
    loads[1].wait()
    loads[2].wait()
    velocity = (mom_ref[...] / dens_ref[...]).reshape(rows, size_z)
    along = jnp.dot(velocity, depth_ref[...], precision=HIGHEST, preferred_element_type=jnp.float32)
    real, imag = along[:, 0:LANES], along[:, LANES:]
    cos_xy = cos_ref[...].reshape(rows, LANES)
    sin_xy = sin_ref[...].reshape(rows, LANES)
    part_cos = jnp.sum(cos_xy * real - sin_xy * imag, axis=0, keepdims=True)
    part_sin = jnp.sum(sin_xy * real + cos_xy * imag, axis=0, keepdims=True)
    both = jnp.concatenate([part_cos, part_sin], axis=0)
    part_ref[:, 0] = jnp.broadcast_to(both[None], (copies, 2, LANES))
    loads[3].wait()
    odd_y = odd("gy_1")
    for n, ref in enumerate((dens_ref, mom_ref, fuel_ref)):
        xlo_ref[n] = ref[0:half]
        xhi_ref[n] = ref[size_x - half : size_x]
    for n, ref in enumerate((mom_ref, fuel_ref)):
        low, high = ref[:, 0:half, :], ref[:, size_y - half : size_y, :]
        sides_ref[n * size_x : (n + 1) * size_x] = jnp.where(odd_y, low, high)
        sides_ref[(n + 2) * size_x : (n + 3) * size_x] = jnp.where(odd_y, high, low)
    turned = [ref[...].reshape(rows, size_z).T for ref in (mom_ref, fuel_ref)]
    low = jnp.concatenate([t[0:half] for t in turned], axis=0)
    high = jnp.concatenate([t[size_z - half : size_z] for t in turned], axis=0)
    following, _ = depth_places()
    for n in range(4):
        pair = slice(2 * n, 2 * n + 2)
        part_ref[:, 1 + n] = jnp.broadcast_to(low[pair][None], (copies, 2, LANES))
        part_ref[pl.ds(following, 1), 1 + n] = high[pair][None]


def partial_sums(density, momentum, hydrogen, modes, full, copies):
    size_x, size_y, size_z = density.shape
    f32 = jnp.float32
    shapes = (
        (copies, 5, 2, LANES),
        (size_x, size_y, LANES),
        (size_x, size_y, LANES),
        (size_z, 2 * LANES),
        (3, 4, size_y, size_z),
        (3, 4, size_y, size_z),
        (4 * size_x, 4, size_z),
    )
    density, momentum, hydrogen, modes = (
        pltpu.with_memory_space_constraint(f, pltpu.HBM) for f in (density, momentum, hydrogen, modes)
    )
    return pl.pallas_call(
        functools.partial(partial_kernel, full, copies),
        out_shape=[jax.ShapeDtypeStruct(s, f32) for s in shapes],
        in_specs=[pl.BlockSpec(memory_space=pltpu.HBM)] * 4,
        out_specs=[VMEM] * len(shapes),
        scratch_shapes=[pltpu.VMEM(density.shape, f32)] * 3
        + [pltpu.VMEM(modes.shape, modes.dtype), pltpu.SemaphoreType.DMA((4,))],
        compiler_params=pltpu.CompilerParams(vmem_limit_bytes=16 << 20),
        name="partial_sums",
    )(density, momentum, hydrogen, modes)


def spread_kernel(parts_ref, out_ref, before_ref, after_ref):
    total = jnp.sum(parts_ref[:, 0], axis=0, keepdims=True)
    out_ref[...] = jnp.broadcast_to(total, out_ref.shape)
    following, preceding = depth_places()
    for n in range(4):
        pair = slice(2 * n, 2 * n + 2)
        before_ref[pair] = parts_ref[preceding, 1 + n]
        after_ref[pair] = parts_ref[following, 1 + n]


def summed_copies(parts, copies):
    edge = jax.ShapeDtypeStruct((8, LANES), jnp.float32)
    return pl.pallas_call(
        spread_kernel,
        out_shape=[jax.ShapeDtypeStruct((copies, 2, LANES), jnp.float32), edge, edge],
        in_specs=[VMEM],
        out_specs=[VMEM] * 3,
        compiler_params=pltpu.CompilerParams(vmem_limit_bytes=4 << 20),
        name="summed_copies",
    )(parts)


def first_diff(planes, at):
    total = None
    for offset, weight in enumerate(FIRST_COEFFS, 1):
        term = weight * (planes[at + offset] - planes[at - offset])
        total = term if total is None else total + term
    return total


def second_diff(pick):
    total = CENTRE_COEFF * pick(0)
    for offset, weight in enumerate(SECOND_COEFFS, 1):
        total = total + weight * (pick(offset) + pick(-offset))
    return total


def final_kernel(
    ncell, dens_ref, mom_ref, fuel_ref, summed_ref, cos_ref, sin_ref, depth_ref,
    xbefore_ref, xafter_ref, traded_ref, relayed_ref, zbefore_ref, zafter_ref,
    dens_out, mom_out, fuel_out, force_ref,
):
    size_x, size_y, size_z = mom_ref.shape
    rows = size_x * size_y
    total = jnp.sum(summed_ref[...], axis=0) * (1.0 / ncell)
    energy = jnp.sum(total * total)
    scaled = total * (2.0 * FORCE_POWER / (energy + ENERGY_EPS))
    coef_cos, coef_sin = scaled[0:1], scaled[1:2]
    cos_xy = cos_ref[...].reshape(rows, LANES)
    sin_xy = sin_ref[...].reshape(rows, LANES)
    side = jnp.concatenate(
        [coef_cos * cos_xy + coef_sin * sin_xy, coef_sin * cos_xy - coef_cos * sin_xy], axis=1
    )
    force_ref[...] = lax.dot_general(
        side, depth_ref[...], (((1,), (1,)), ((), ())), precision=HIGHEST,
        preferred_element_type=jnp.float32,
    ).reshape(size_x, size_y, size_z)
    gap = jnp.zeros((56, rows), jnp.float32)
    odd_y = odd("gy_1")
    before, after = zbefore_ref[...], zafter_ref[...]
    turned = jnp.concatenate(
        [after[0:4], gap, before[4:8], after[4:8], gap, before[0:4]], axis=0
    ).T
    halo = [turned, pltpu.roll(turned, 64, 1)]
    lane = lax.broadcasted_iota(jnp.int32, (1, size_z), 1)
    dens, mom, fuel = (
        [xbefore_ref[n, i] for i in range(4)] + [ref[i] for i in range(size_x)] + [xafter_ref[n, i] for i in range(4)]
        for n, ref in enumerate((dens_ref, mom_ref, fuel_ref))
    )
    vel = [m / d for m, d in zip(mom, dens)]
    mom_flux = [m * v + d for m, v, d in zip(mom, vel, dens)]
    fuel_flux = [f * v for f, v in zip(fuel, vel)]
    for i in range(size_x):
        at = i + 4
        dens_out[i] = -first_diff(mom, at)
        spread = []
        for n, planes in enumerate((mom, fuel)):
            here = planes[at]
            ya, yb = traded_ref[n * size_x + i], relayed_ref[n * size_x + i]
            tall = jnp.concatenate([jnp.where(odd_y, ya, yb), here, jnp.where(odd_y, yb, ya)], axis=0)
            edge = halo[n][i * size_y : (i + 1) * size_y]

            def along_z(offset):
                if offset == 0:
                    return here
                if offset > 0:
                    return pltpu.roll(jnp.where(lane < offset, edge, here), size_z - offset, 1)
                return pltpu.roll(jnp.where(lane >= size_z + offset, edge, here), -offset, 1)

            spread.append(
                second_diff(lambda o: planes[at + o])
                + second_diff(lambda o: tall[4 + o : 4 + o + size_y])
                + second_diff(along_z)
            )
        mom_out[i] = -first_diff(mom_flux, at) + VISCOSITY * spread[0] + dens[at] * force_ref[i]
        fuel_out[i] = (
            -first_diff(fuel_flux, at) + DIFFUSIVITY * spread[1]
            - fuel[at] * jnp.exp(-ACTIVATION * fuel[at] / dens[at])
        )


def final_rates(density, momentum, hydrogen, summed, cos, sin, depth, halos, ncell):
    shape = density.shape
    return pl.pallas_call(
        functools.partial(final_kernel, ncell),
        out_shape=[jax.ShapeDtypeStruct(shape, jnp.float32)] * 3,
        in_specs=[VMEM] * 13,
        out_specs=[VMEM] * 3,
        scratch_shapes=[pltpu.VMEM(shape, jnp.float32)],
        compiler_params=pltpu.CompilerParams(vmem_limit_bytes=16 << 20),
        name="final_rates",
    )(density, momentum, hydrogen, summed, cos, sin, depth, *halos)


def shift(x, axes, by):
    size = lax.axis_size(axes)
    return lax.ppermute(x, axes, [(i, (i + by) % size) for i in range(size)])


def swap(x, axes, shift):
    size = lax.axis_size(axes)
    pairs = [((i + shift) % size, (i + 1 + shift) % size) for i in range(0, size, 2)]
    return lax.ppermute(x, axes, pairs + [(j, i) for i, j in pairs])


def relay(x):
    size = lax.axis_size("gy_0")
    ups = [(2 * i, 2 * ((i + 1) % size)) for i in range(size)]
    downs = [(2 * i + 1, 2 * ((i - 1) % size) + 1) for i in range(size)]
    return lax.ppermute(x, GY, ups + downs)


def exchange(x, axes, groups=None):
    return lax.all_to_all(x, axes, 0, 0, axis_index_groups=groups, tiled=True)


def per_device(density, momentum, hydrogen, forced_modes):
    size_x, size_y, size_z = density.shape
    full = (
        size_x * lax.axis_size(GX),
        size_y * lax.axis_size(GY),
        size_z * lax.axis_size(GZ),
    )
    first, second = lax.axis_size(FIRST_GROUP), lax.axis_size(SECOND_GROUP)
    part, cos, sin, depth, xlo, xhi, sides = partial_sums(
        density, momentum, hydrogen, forced_modes.T, full, first
    )
    order = [(FIRST_MEMBER + i) % first for i in range(first)]
    part = exchange(part, FIRST_GROUP, [order])
    traded = swap(sides, ("gy_1",), 0)
    part, zbefore, zafter = summed_copies(part, second)
    part = exchange(part, SECOND_GROUP)
    xbefore, xafter = shift(xhi, GX, 1), shift(xlo, GX, -1)
    relayed = relay(traded[2 * size_x : 4 * size_x])
    rates = final_rates(
        density, momentum, hydrogen, part, cos, sin, depth,
        (xbefore, xafter, traded, relayed, zbefore, zafter), float(full[0] * full[1] * full[2]),
    )
    return tuple(rates)


def solution(mesh):
    split = Mesh(
        mesh.devices.reshape(8, 2, 4, 2, mesh.shape["gz"]), ("gx_0", "gx_1", "gy_0", "gy_1", "gz")
    )
    field = P(GX, GY, "gz")
    return jax.shard_map(
        per_device, mesh=split, in_specs=(field, field, field, P()),
        out_specs=(field, field, field), check_vma=False,
    )
```

```python
import functools

import jax
import jax.numpy as jnp
from jax import lax
from jax.experimental import pallas as pl
from jax.experimental.pallas import tpu as pltpu
from jax.sharding import Mesh
from jax.sharding import PartitionSpec as P


GX = ("gx_0", "gx_1")
GY = ("gy_0", "gy_1")
GZ = ("gz",)
FIRST_GROUP = ("gy_1", "gz")
FIRST_MEMBER = 8
PLANE_MEMBER = 32
SECOND_GROUP = ("gx_0", "gx_1", "gy_0")

FIRST_COEFFS = (0.8, -0.2, 4.0 / 105.0, -1.0 / 280.0)
SECOND_COEFFS = (1.6, -0.2, 8.0 / 315.0, -1.0 / 560.0)
CENTRE_COEFF = -205.0 / 72.0
VISCOSITY = 0.3
DIFFUSIVITY = 1.5
FORCE_POWER = 0.3
ENERGY_EPS = 1e-06
ACTIVATION = 2.0
HIGHEST = lax.Precision.HIGHEST
LANES = 128
VMEM = pl.BlockSpec(memory_space=pltpu.VMEM)


def odd(axis):
    return lax.rem(lax.axis_index(axis), 2) == 1


def depth_places():
    place, count = lax.axis_index("gz"), lax.axis_size("gz")
    whole = count * lax.axis_size("gy_1")
    base = lax.axis_index("gy_1") * count + whole - FIRST_MEMBER
    return tuple(lax.rem(base + lax.rem(place + by, count), whole) for by in (1, count - 1))


def angles(wave, start, step, count, total):
    index = lax.broadcasted_iota(jnp.int32, (count, LANES), 0)
    position = (start + step * index).astype(jnp.float32)
    phase = wave * position
    phase = phase - total * jnp.round(phase * (1.0 / total))
    return (2.0 * jnp.pi / total) * phase


def partial_kernel(
    full, copies, dens_hbm, mom_hbm, fuel_hbm, modes_hbm,
    part_ref, cos_ref, sin_ref, depth_ref,
    xlo_ref, xhi_ref, sides_ref,
    dens_ref, mom_ref, fuel_ref, modes_ref, sems,
):
    size_x, size_y, size_z = mom_ref.shape
    rows = size_x * size_y
    half = 4
    loads = [
        pltpu.make_async_copy(src, dst, sems.at[n])
        for n, (src, dst) in enumerate(
            ((modes_hbm, modes_ref), (mom_hbm, mom_ref), (dens_hbm, dens_ref), (fuel_hbm, fuel_ref))
        )
    ]
    for load in loads:
        load.start()
    loads[0].wait()
    modes = modes_ref[...].astype(jnp.float32)
    spare = jnp.zeros((1, LANES - modes.shape[1]), jnp.float32)
    wave_x, wave_y, wave_z = (jnp.concatenate([modes[n : n + 1], spare], axis=1) for n in range(3))
    base_x = (lax.axis_index("gx_0") * 2 + lax.axis_index("gx_1")) * size_x
    base_y = (lax.axis_index("gy_0") * 2 + lax.axis_index("gy_1")) * size_y
    base_z = lax.axis_index("gz") * size_z
    fine = size_z // 8
    angle = jnp.concatenate(
        [
            angles(wave_x, base_x, 1, size_x, full[0]),
            angles(wave_y, base_y, 1, size_y, full[1]),
            angles(wave_z, base_z, fine, 8, full[2]),
            angles(wave_z, 0, 1, fine, full[2]),
        ],
        axis=0,
    )
    cos, sin = jnp.cos(angle), jnp.sin(angle)
    at_y, at_z, at_f = size_x, size_x + size_y, size_x + size_y + 8
    cy, sy = cos[at_y:at_z], sin[at_y:at_z]
    live = lax.broadcasted_iota(jnp.int32, (1, LANES), 1) < modes.shape[1]
    cf = jnp.where(live, cos[at_f:], 0.0)
    sf = jnp.where(live, sin[at_f:], 0.0)
    for n in range(size_x):
        cx, sx = cos[n : n + 1], sin[n : n + 1]
        cos_ref[n] = cx * cy - sx * sy
        sin_ref[n] = sx * cy + cx * sy
    for n in range(8):
        cz, sz = cos[at_z + n : at_z + n + 1], sin[at_z + n : at_z + n + 1]
        depth_ref[n * fine : (n + 1) * fine, 0:LANES] = cz * cf - sz * sf
        depth_ref[n * fine : (n + 1) * fine, LANES:] = sz * cf + cz * sf
    loads[1].wait()
    loads[2].wait()
    velocity = (mom_ref[...] / dens_ref[...]).reshape(rows, size_z)
    along = jnp.dot(velocity, depth_ref[...], precision=HIGHEST, preferred_element_type=jnp.float32)
    real, imag = along[:, 0:LANES], along[:, LANES:]
    cos_xy = cos_ref[...].reshape(rows, LANES)
    sin_xy = sin_ref[...].reshape(rows, LANES)
    part_cos = jnp.sum(cos_xy * real - sin_xy * imag, axis=0, keepdims=True)
    part_sin = jnp.sum(sin_xy * real + cos_xy * imag, axis=0, keepdims=True)
    both = jnp.concatenate([part_cos, part_sin], axis=0)
    part_ref[:, 0] = jnp.broadcast_to(both[None], (copies, 2, LANES))
    loads[3].wait()
    odd_y = odd("gy_1")
    for n, ref in enumerate((dens_ref, mom_ref, fuel_ref)):
        xlo_ref[n] = ref[0:half]
        xhi_ref[n] = ref[size_x - half : size_x]
    for n, ref in enumerate((mom_ref, fuel_ref)):
        low, high = ref[:, 0:half, :], ref[:, size_y - half : size_y, :]
        sides_ref[n * size_x : (n + 1) * size_x] = jnp.where(odd_y, low, high)
        sides_ref[(n + 2) * size_x : (n + 3) * size_x] = jnp.where(odd_y, high, low)
    turned = [ref[...].reshape(rows, size_z).T for ref in (mom_ref, fuel_ref)]
    low = jnp.concatenate([t[0:half] for t in turned], axis=0)
    high = jnp.concatenate([t[size_z - half : size_z] for t in turned], axis=0)
    following, _ = depth_places()
    for n in range(4):
        pair = slice(2 * n, 2 * n + 2)
        part_ref[:, 1 + n] = jnp.broadcast_to(low[pair][None], (copies, 2, LANES))
        part_ref[pl.ds(following, 1), 1 + n] = high[pair][None]


def partial_sums(density, momentum, hydrogen, modes, full, copies):
    size_x, size_y, size_z = density.shape
    f32 = jnp.float32
    shapes = (
        (copies, 5, 2, LANES),
        (size_x, size_y, LANES),
        (size_x, size_y, LANES),
        (size_z, 2 * LANES),
        (3, 4, size_y, size_z),
        (3, 4, size_y, size_z),
        (4 * size_x, 4, size_z),
    )
    density, momentum, hydrogen, modes = (
        pltpu.with_memory_space_constraint(f, pltpu.HBM) for f in (density, momentum, hydrogen, modes)
    )
    return pl.pallas_call(
        functools.partial(partial_kernel, full, copies),
        out_shape=[jax.ShapeDtypeStruct(s, f32) for s in shapes],
        in_specs=[pl.BlockSpec(memory_space=pltpu.HBM)] * 4,
        out_specs=[VMEM] * len(shapes),
        scratch_shapes=[pltpu.VMEM(density.shape, f32)] * 3
        + [pltpu.VMEM(modes.shape, modes.dtype), pltpu.SemaphoreType.DMA((4,))],
        compiler_params=pltpu.CompilerParams(vmem_limit_bytes=16 << 20),
        name="partial_sums",
    )(density, momentum, hydrogen, modes)


def spread_kernel(parts_ref, out_ref, before_ref, after_ref):
    total = jnp.sum(parts_ref[:, 0], axis=0, keepdims=True)
    out_ref[...] = jnp.broadcast_to(total, out_ref.shape)
    following, preceding = depth_places()
    for n in range(4):
        pair = slice(2 * n, 2 * n + 2)
        before_ref[pair] = parts_ref[preceding, 1 + n]
        after_ref[pair] = parts_ref[following, 1 + n]


def summed_copies(parts, copies):
    edge = jax.ShapeDtypeStruct((8, LANES), jnp.float32)
    return pl.pallas_call(
        spread_kernel,
        out_shape=[jax.ShapeDtypeStruct((copies, 2, LANES), jnp.float32), edge, edge],
        in_specs=[VMEM],
        out_specs=[VMEM] * 3,
        compiler_params=pltpu.CompilerParams(vmem_limit_bytes=4 << 20),
        name="summed_copies",
    )(parts)


def first_diff(planes, at):
    total = None
    for offset, weight in enumerate(FIRST_COEFFS, 1):
        term = weight * (planes[at + offset] - planes[at - offset])
        total = term if total is None else total + term
    return total


def second_diff(pick):
    total = CENTRE_COEFF * pick(0)
    for offset, weight in enumerate(SECOND_COEFFS, 1):
        total = total + weight * (pick(offset) + pick(-offset))
    return total


def final_kernel(
    ncell, dens_ref, mom_ref, fuel_ref, summed_ref, cos_ref, sin_ref, depth_ref,
    xbefore_ref, xafter_ref, traded_ref, relayed_ref, zbefore_ref, zafter_ref,
    dens_out, mom_out, fuel_out, force_ref,
):
    size_x, size_y, size_z = mom_ref.shape
    rows = size_x * size_y
    total = jnp.sum(summed_ref[...], axis=0) * (1.0 / ncell)
    energy = jnp.sum(total * total)
    scaled = total * (2.0 * FORCE_POWER / (energy + ENERGY_EPS))
    coef_cos, coef_sin = scaled[0:1], scaled[1:2]
    cos_xy = cos_ref[...].reshape(rows, LANES)
    sin_xy = sin_ref[...].reshape(rows, LANES)
    side = jnp.concatenate(
        [coef_cos * cos_xy + coef_sin * sin_xy, coef_sin * cos_xy - coef_cos * sin_xy], axis=1
    )
    force_ref[...] = lax.dot_general(
        side, depth_ref[...], (((1,), (1,)), ((), ())), precision=HIGHEST,
        preferred_element_type=jnp.float32,
    ).reshape(size_x, size_y, size_z)
    gap = jnp.zeros((56, rows), jnp.float32)
    odd_y = odd("gy_1")
    before, after = zbefore_ref[...], zafter_ref[...]
    turned = jnp.concatenate(
        [after[0:4], gap, before[4:8], after[4:8], gap, before[0:4]], axis=0
    ).T
    halo = [turned, pltpu.roll(turned, 64, 1)]
    lane = lax.broadcasted_iota(jnp.int32, (1, size_z), 1)
    dens, mom, fuel = (
        [xbefore_ref[n, i] for i in range(4)] + [ref[i] for i in range(size_x)] + [xafter_ref[n, i] for i in range(4)]
        for n, ref in enumerate((dens_ref, mom_ref, fuel_ref))
    )
    vel = [m / d for m, d in zip(mom, dens)]
    mom_flux = [m * v + d for m, v, d in zip(mom, vel, dens)]
    fuel_flux = [f * v for f, v in zip(fuel, vel)]
    for i in range(size_x):
        at = i + 4
        dens_out[i] = -first_diff(mom, at)
        spread = []
        for n, planes in enumerate((mom, fuel)):
            here = planes[at]
            ya, yb = traded_ref[n * size_x + i], relayed_ref[n * size_x + i]
            tall = jnp.concatenate([jnp.where(odd_y, ya, yb), here, jnp.where(odd_y, yb, ya)], axis=0)
            edge = halo[n][i * size_y : (i + 1) * size_y]

            def along_z(offset):
                if offset == 0:
                    return here
                if offset > 0:
                    return pltpu.roll(jnp.where(lane < offset, edge, here), size_z - offset, 1)
                return pltpu.roll(jnp.where(lane >= size_z + offset, edge, here), -offset, 1)

            spread.append(
                second_diff(lambda o: planes[at + o])
                + second_diff(lambda o: tall[4 + o : 4 + o + size_y])
                + second_diff(along_z)
            )
        mom_out[i] = -first_diff(mom_flux, at) + VISCOSITY * spread[0] + dens[at] * force_ref[i]
        fuel_out[i] = (
            -first_diff(fuel_flux, at) + DIFFUSIVITY * spread[1]
            - fuel[at] * jnp.exp(-ACTIVATION * fuel[at] / dens[at])
        )


def final_rates(density, momentum, hydrogen, summed, cos, sin, depth, halos, ncell):
    shape = density.shape
    return pl.pallas_call(
        functools.partial(final_kernel, ncell),
        out_shape=[jax.ShapeDtypeStruct(shape, jnp.float32)] * 3,
        in_specs=[VMEM] * 13,
        out_specs=[VMEM] * 3,
        scratch_shapes=[pltpu.VMEM(shape, jnp.float32)],
        compiler_params=pltpu.CompilerParams(vmem_limit_bytes=16 << 20),
        name="final_rates",
    )(density, momentum, hydrogen, summed, cos, sin, depth, *halos)


def shift(x, axes, by):
    size = lax.axis_size(axes)
    return lax.ppermute(x, axes, [(i, (i + by) % size) for i in range(size)])


def swap(x, axes, shift):
    size = lax.axis_size(axes)
    pairs = [((i + shift) % size, (i + 1 + shift) % size) for i in range(0, size, 2)]
    return lax.ppermute(x, axes, pairs + [(j, i) for i, j in pairs])


def relay(x):
    size = lax.axis_size("gy_0")
    ups = [(2 * i, 2 * ((i + 1) % size)) for i in range(size)]
    downs = [(2 * i + 1, 2 * ((i - 1) % size) + 1) for i in range(size)]
    return lax.ppermute(x, GY, ups + downs)


def exchange(x, axes, member):
    size = lax.axis_size(axes)
    order = [(member + i) % size for i in range(size)]
    return lax.all_to_all(x, axes, 0, 0, axis_index_groups=[order], tiled=True)


def per_device(density, momentum, hydrogen, forced_modes):
    size_x, size_y, size_z = density.shape
    full = (
        size_x * lax.axis_size(GX),
        size_y * lax.axis_size(GY),
        size_z * lax.axis_size(GZ),
    )
    first, second = lax.axis_size(FIRST_GROUP), lax.axis_size(SECOND_GROUP)
    part, cos, sin, depth, xlo, xhi, sides = partial_sums(
        density, momentum, hydrogen, forced_modes.T, full, first
    )
    part = exchange(part, FIRST_GROUP, FIRST_MEMBER)
    traded = swap(sides, ("gy_1",), 0)
    xbefore, xafter = shift(xhi, GX, 1), shift(xlo, GX, -1)
    part, zbefore, zafter = summed_copies(part, second)
    part = exchange(part, SECOND_GROUP, PLANE_MEMBER)
    relayed = relay(traded[2 * size_x : 4 * size_x])
    rates = final_rates(
        density, momentum, hydrogen, part, cos, sin, depth,
        (xbefore, xafter, traded, relayed, zbefore, zafter), float(full[0] * full[1] * full[2]),
    )
    return tuple(rates)


def solution(mesh):
    split = Mesh(
        mesh.devices.reshape(8, 2, 4, 2, mesh.shape["gz"]), ("gx_0", "gx_1", "gy_0", "gy_1", "gz")
    )
    field = P(GX, GY, "gz")
    return jax.shard_map(
        per_device, mesh=split, in_specs=(field, field, field, P()),
        out_specs=(field, field, field), check_vma=False,
    )
```
